32 devices in a mesh: row: 2 (over core), col: 16 (over z, y, x).
Axes of the slice: x: 2, y: 2, z: 4, core: 2. Of those that a mesh axis runs over, the one named last changes fastest.
Arguments:
- observed: bfloat16 [1024, 16, 2048], P(None, 'row', 'col'), may hold values from -40 to 40
- library: bfloat16 [1024, 256], P('col'), may hold values from -0.1875 to 0.1875
Outputs:
- abundance: float32 [256, 16, 2048], P(None, 'row', 'col')
The draws below stay inside these ranges and needn't reach their ends.
All inputs are finite; a program needn't handle non-finite values.
Results may differ from the reference program's by a relative error of at most 0.0024.
Values may be sent and summed in bfloat16 or wider, within the bound.
No kernel may reach another device: no remote copies, remote signals or barrier semaphores. Data moves between devices by JAX's collectives and lax.ppermute only.
A program may use at most 128 MiB of HBM per device.

```python
import jax
import jax.numpy as jnp
from jax import lax

CHANNELS = 1024
ENDMEMBERS = 256
ITERS = 3
ROWS = 16
COLS = 2048


def draw_observed(key, part):
    subkeys = jax.random.split(jax.random.fold_in(key, 17), 4)
    shape = (CHANNELS, ROWS, COLS)
    noise_base = jax.random.normal(subkeys[0], shape, jnp.float32)
    region_low, region_high = (jnp.log(1.0 / 3.0), jnp.log(3.0))
    channel_scale = jnp.exp(jax.random.uniform(subkeys[1], (CHANNELS, 1, 1), jnp.float32, jnp.log(0.5), jnp.log(2.0)))
    region_table = jnp.exp(jax.random.uniform(subkeys[2], (COLS // 32,), jnp.float32, region_low, region_high))
    region_scale = jnp.repeat(region_table, 32).reshape(1, 1, COLS)
    pixel_scale = jax.random.uniform(subkeys[3], (1, ROWS, COLS), jnp.float32, 0.5, 1.5)
    return jnp.clip(noise_base * channel_scale * region_scale * pixel_scale, -40.0, 40.0).astype(jnp.bfloat16)


def steps_of(rng, dims, cuts, smallest, high):
    def one(dim, shards_of):
        draws = jax.random.uniform(jax.random.fold_in(jax.random.fold_in(rng, 6), dim), (shards_of,), jnp.float32, smallest / len(cuts), high / len(cuts))
        return jnp.repeat(jnp.exp(draws), dims[dim] // shards_of).reshape((-1,) + (1,) * (len(dims) - dim - 1))

    level = one(*cuts[0])
    for cut in cuts[1:]:
        level = level * one(*cut)
    return level


def noise(rng, extent, deviation, limit, shards=(), held_as=jnp.bfloat16):
    result = deviation * jax.random.normal(rng, extent, jnp.float32)
    if shards:
        result = result * steps_of(rng, extent, shards, -0.22, 0.18)
    return jnp.clip(result, -limit, limit).astype(held_as)


def setup_inputs(seed: int = 0) -> dict:
    splits = jax.random.split(jax.random.key(seed), 3)
    observed = draw_observed(jax.random.fold_in(splits[2], 71), 0)
    library = noise(splits[1], (CHANNELS, ENDMEMBERS), CHANNELS ** -0.5, 0.1875, ((0, 16),))
    return {"observed": observed, "library": library}


prox_tau = 8.0
weight_sparse = 0.3
weight_tv = 1.0

def soften(values_in, threshold):
    return values_in - jnp.clip(values_in, -threshold, threshold)

def gradient(field_in):
    zero_row = jnp.zeros_like(field_in[:, :1, :])
    zero_col = jnp.zeros_like(field_in[:, :, :1])
    down_diff = jnp.concatenate([field_in[:, 1:, :] - field_in[:, :-1, :], zero_row], axis=1)
    right_diff = jnp.concatenate([field_in[:, :, 1:] - field_in[:, :, :-1], zero_col], axis=2)
    return (down_diff, right_diff)

def adjoint(down_arg, right_arg):
    zero_row = jnp.zeros_like(down_arg[:, :1, :])
    zero_col = jnp.zeros_like(right_arg[:, :, :1])
    down_kept = jnp.concatenate([down_arg[:, :-1, :], zero_row], axis=1)
    right_kept = jnp.concatenate([right_arg[:, :, :-1], zero_col], axis=2)
    upper_part = jnp.concatenate([zero_row, down_kept[:, :-1, :]], axis=1)
    side_part = jnp.concatenate([zero_col, right_kept[:, :, :-1]], axis=2)
    return upper_part - down_kept + (side_part - right_kept)

def solve_step(library, inverse, estimate, data_var, data_dual, sparse_var, sparse_dual, diverge):
    packed = (data_var - data_dual).astype(jnp.bfloat16).reshape(CHANNELS, -1)
    projected = jnp.dot(library.T.astype(jnp.float32), packed.astype(jnp.float32), preferred_element_type=jnp.float32).reshape(estimate.shape)
    rhs_field = projected + (sparse_var - sparse_dual) + prox_tau * estimate - diverge
    solved = jnp.dot(inverse, rhs_field.reshape(ENDMEMBERS, -1), precision=lax.Precision.HIGHEST)
    return solved.reshape(estimate.shape)

def reference(observed, library):
    gram_matrix = jnp.dot(library.T.astype(jnp.float32), library.astype(jnp.float32), preferred_element_type=jnp.float32)
    identity = jnp.eye(ENDMEMBERS, dtype=jnp.float32)
    system = gram_matrix + (1.0 + prox_tau) * identity
    factor = jnp.linalg.cholesky(system)
    inverse = jax.scipy.linalg.cho_solve((factor, True), identity)
    observed_wide = observed.astype(jnp.float32)
    data_var = observed_wide
    data_dual = jnp.zeros_like(observed_wide)
    estimate = jnp.zeros((ENDMEMBERS, ROWS, COLS), jnp.float32)
    sparse_var = jnp.zeros_like(estimate)
    sparse_dual = jnp.zeros_like(estimate)
    down_var = jnp.zeros_like(estimate)
    right_var = jnp.zeros_like(estimate)
    down_dual = jnp.zeros_like(estimate)
    right_dual = jnp.zeros_like(estimate)
    diverge = jnp.zeros_like(estimate)
    penalty = jnp.float32(1.0)
    for iteration in range(ITERS):
        estimate = solve_step(library, inverse, estimate, data_var, data_dual, sparse_var, sparse_dual, diverge)
        half_estimate = estimate.astype(jnp.bfloat16).reshape(ENDMEMBERS, -1)
        modelled = jnp.dot(library.astype(jnp.float32), half_estimate.astype(jnp.float32), preferred_element_type=jnp.float32).reshape(observed.shape)
        down_diff, right_diff = gradient(estimate)
        data_var = (observed_wide + penalty * (modelled + data_dual)) / (1.0 + penalty)
        new_sparse = jnp.maximum(estimate + sparse_dual - weight_sparse / penalty, 0.0)
        new_down = soften(down_diff + down_dual, weight_tv / penalty)
        new_right = soften(right_diff + right_dual, weight_tv / penalty)
        data_dual = data_dual + modelled - data_var
        sparse_dual = sparse_dual + estimate - new_sparse
        down_dual = down_dual + down_diff - new_down
        right_dual = right_dual + right_diff - new_right
        primal = jnp.sum((modelled - data_var) ** 2) + jnp.sum((estimate - new_sparse) ** 2) + jnp.sum((down_diff - new_down) ** 2) + jnp.sum((right_diff - new_right) ** 2)
        dual_sum = jnp.sum((new_sparse - sparse_var) ** 2) + jnp.sum((new_down - down_var) ** 2) + jnp.sum((new_right - right_var) ** 2)
        sparse_var, down_var, right_var = (new_sparse, new_down, new_right)
        following = penalty * jnp.sqrt(jnp.sqrt((primal + 1.0) / (penalty * penalty * dual_sum + 1.0)))
        rescale = penalty / following
        data_dual = data_dual * rescale
        sparse_dual = sparse_dual * rescale
        down_dual = down_dual * rescale
        right_dual = right_dual * rescale
        penalty = following
        diverge = adjoint(down_diff - down_var + down_dual, right_diff - right_var + right_dual)
    estimate = solve_step(library, inverse, estimate, data_var, data_dual, sparse_var, sparse_dual, diverge)
    return estimate
```

```python
import functools

import jax
import jax.numpy as jnp
from jax import lax
from jax.experimental import pallas as pl
from jax.experimental.pallas import tpu as pltpu
from jax.sharding import PartitionSpec as P

ITERS = 3

prox_tau = 8.0
weight_sparse = 0.3
weight_tv = 1.0

F32 = jnp.float32
BF16 = jnp.bfloat16
SHIFT = 1.0 + prox_tau
GROUP = 8
UNROLL = 16


def split(value):
    high = value.astype(BF16)
    return high, (value - high.astype(F32)).astype(BF16)


def dot(left, right):
    return jnp.dot(left, right, preferred_element_type=F32)


def dot_full(left, right):
    return jnp.dot(left, right, precision=lax.Precision.HIGHEST, preferred_element_type=F32)


def dot_columns(left, right):
    return lax.dot_general(left, right, (((0,), (0,)), ((), ())), preferred_element_type=F32)


def clip(value, bound):
    return jnp.minimum(jnp.maximum(value, -bound), bound)


def call(body, outs, args, scratch=(), flops=0, limit=24):
    return pl.pallas_call(
        body,
        out_shape=[jax.ShapeDtypeStruct(*out) for out in outs],
        in_specs=[pl.BlockSpec(memory_space=pltpu.VMEM)] * len(args),
        out_specs=[pl.BlockSpec(memory_space=pltpu.VMEM)] * len(outs),
        scratch_shapes=list(scratch),
        cost_estimate=pl.CostEstimate(flops=flops, bytes_accessed=0, transcendentals=0),
        compiler_params=pltpu.CompilerParams(vmem_limit_bytes=limit << 20),
    )(*args)


def groups(members, step):
    def body(index, carry):
        return step(pl.multiple_of(index * GROUP, GROUP), carry)

    return body, members // GROUP


def roll(value, shift):
    return pltpu.roll(value, shift % value.shape[1], 1)


def lanes_of(shape):
    return lax.broadcasted_iota(jnp.int32, shape, 1)


def flag(condition):
    return jnp.where(condition, 1.0, 0.0).astype(F32)


def edge_flags():
    row, col = lax.axis_index("row"), lax.axis_index("col")
    return (
        flag(row > 0),
        flag(row < lax.axis_size("row") - 1),
        flag(col > 0),
        flag(col < lax.axis_size("col") - 1),
    )


def invert(gram, inverse, power, left):
    eye = flag(
        lax.broadcasted_iota(jnp.int32, gram.shape, 0) == lax.broadcasted_iota(jnp.int32, gram.shape, 1)
    )
    system = gram + SHIFT * eye
    bound = jnp.max(jnp.sum(jnp.abs(gram), axis=1, keepdims=True)) + SHIFT
    nearest = jnp.sum(system * eye) / jnp.sum(system * system)
    scale = jnp.where(nearest * bound < 1.9, nearest, 2.0 / (bound + SHIFT))
    first = eye - scale * system
    squared = dot_full(first, first)
    inverse[...] = scale * (eye + first)
    power[...] = squared
    left[0] = jnp.sum(squared * squared)

    def step(index, carry):
        @pl.when(left[0] > 0.0)
        def _():
            current = power[...]
            inverse[...] = inverse[...] + dot_full(inverse[...], current)

        @pl.when(left[0] > 1e-6)
        def _():
            current = power[...]
            squared = dot_full(current, current)
            power[...] = squared
            left[1] = jnp.sum(squared * squared)

        left[0] = jnp.where(left[0] > 1e-6, left[1], 0.0)
        return carry

    lax.fori_loop(0, 20, step, 0)


def apply_inverse(inv_high, inv_low, rhs_high, rhs_low, store):
    width = rhs_high.shape[1]
    for start in range(0, width, 512):
        block = min(512, width - start)
        high, low = rhs_high[:, start : start + block], rhs_low[:, start : start + block]
        store(start, block, dot(inv_high[...], high) + (dot(inv_high[...], low) + dot(inv_low[...], high)))


def survey_kernel(rows, cols, observed, columns, row_edge, norm):
    channels, pixels = observed.shape
    spot = lax.broadcasted_iota(jnp.int32, (2 * rows, pixels), 0)
    pixel = lax.broadcasted_iota(jnp.int32, (2 * rows, pixels), 1)
    wanted = jnp.where(spot < rows, spot * cols, (spot - rows) * cols + cols - 1)
    chosen = flag(pixel == wanted).astype(BF16)
    columns[...] = lax.dot_general(
        chosen, observed[...], (((1,), (1,)), ((), ())), preferred_element_type=F32
    ).astype(BF16)
    is_upper = edge_flags()[1] > 0.0

    @pl.when(is_upper)
    def _():
        row_edge[...] = observed[:, pixels - cols :]

    @pl.when(jnp.logical_not(is_upper))
    def _():
        row_edge[...] = observed[:, :cols]

    tall = 2 * GROUP

    def step(index, total):
        here = pl.ds(pl.multiple_of(index * tall, tall), tall)
        total = list(total)
        for i in range(rows):
            value = observed[here, i * cols : (i + 1) * cols].astype(F32)
            total[i % 2] = total[i % 2] + value * value
        return tuple(total)

    zero = jnp.zeros((tall, cols), F32)
    even, odd = lax.fori_loop(0, channels // tall, step, (zero, zero), unroll=8)
    total = even + odd
    norm[...] = total[:GROUP, :] + total[GROUP:, :]


def start_kernel(rows, cols, order, *refs):
    ordered = order is True
    observed, row_halo, left_halo, right_halo = refs[:4]
    inputs = 5 if ordered else 9
    pieces = refs[4:inputs]
    projected, inv_high, inv_low, fit, fit_gram, quad, near_row, near_left, near_right = refs[inputs : inputs + 9]
    inverse, power, rhs_high, rhs_low, left, panel = refs[inputs + 9 : inputs + 15]
    if ordered:
        full = pieces[0]
    else:
        full = refs[inputs + 15]
        place_library(pieces, full, order)
    members = full.shape[1]
    pixels = rows * cols
    panel[...] = jnp.zeros(panel.shape, BF16)
    panel[0 : 2 * rows, :] = right_halo[...]
    panel[2 * rows : 4 * rows, :] = left_halo[...]
    block = min(512, pixels)
    for start in range(0, pixels, block):
        span = slice(start, start + block)
        result = dot_columns(full[...], observed[:, span])
        projected[:, span] = result
        rhs_high[:, span], rhs_low[:, span] = split(result)
    span = slice(pixels, pixels + cols)
    rhs_high[:, span], rhs_low[:, span] = split(dot_columns(full[...], row_halo[...]))
    span = slice(pixels + cols, pixels + cols + panel.shape[0])
    beside = lax.dot_general(full[...], panel[...], (((0,), (1,)), ((), ())), preferred_element_type=F32)
    rhs_high[:, span], rhs_low[:, span] = split(beside)
    invert(dot_columns(full[...], full[...]), inverse, power, left)
    inv_high[...], inv_low[...] = split(inverse[...])

    def store(start, size, value):
        if start < pixels:
            fit[:, start : start + size] = value
        else:
            near_row[...] = value[:, :cols]
            near_right[...] = value[:, cols:]
            near_left[...] = roll(value[:, cols:], -3 * rows)

    apply_inverse(inv_high, inv_low, rhs_high, rhs_low, store)

    def step(base, sums):
        here = pl.ds(base, GROUP)
        total, cross = sums
        for i in range(rows):
            span = slice(i * cols, (i + 1) * cols)
            a, p = fit[here, span], projected[here, span]
            ga = p - SHIFT * a
            fit_gram[here, span] = ga
            total = total + a * (ga - 2.0 * p)
            cross = cross + a * p
        return total, cross

    zero = jnp.zeros((GROUP, cols), F32)
    body, count = groups(members, step)
    total, cross = lax.fori_loop(0, count, body, (zero, zero), unroll=UNROLL)
    quad[0:GROUP, :] = total
    quad[GROUP : 2 * GROUP, :] = cross


def write_edges(base, members, a, b, below, row_edge, left_edge, right_edge):
    here = pl.ds(base, GROUP)
    is_upper = below > 0.0
    row_edge[here, :] = jnp.where(is_upper, a[-1], a[0])
    row_edge[pl.ds(base + members, GROUP), :] = jnp.where(is_upper, b[-1], b[0])
    lane = lanes_of(a[0].shape)
    cols = a[0].shape[1]
    left = jnp.zeros_like(a[0])
    right = jnp.zeros_like(a[0])
    for i, value in enumerate(a + b):
        left = jnp.where(lane == i, roll(value, i), left)
        right = jnp.where(lane == i, roll(value, i + 1 - cols), right)
    left_edge[here, :] = left
    right_edge[here, :] = right


def place_library(pieces, full, order):
    mine, mine_rest, other, other_rest, rows_of = pieces
    rows = rows_of.shape[0]
    own = lax.axis_index("col")
    parity = lax.axis_index("row")
    bits = own
    for _ in range(max(1, (lax.axis_size("col") - 1).bit_length())):
        parity = parity ^ (bits & 1)
        bits = bits >> 1
    half = parity
    blocks = mine.shape[0] // rows
    for offset, first, second in ((0, mine, other), (blocks, mine_rest, other_rest)):
        for block in range(blocks):
            base = (own ^ order[block + offset]) * (2 * rows)
            source = slice(block * rows, (block + 1) * rows)
            full[pl.ds(pl.multiple_of(base + half * rows, rows), rows), :] = first[source, :]
            full[pl.ds(pl.multiple_of(base + (1 - half) * rows, rows), rows), :] = second[source, :]


def new_penalty(scalars, sums):
    penalty = scalars[0:1, 0:1]
    primal = jnp.sum(jnp.sum(sums[0:GROUP, :], axis=0, keepdims=True), axis=1, keepdims=True)
    dual = jnp.sum(jnp.sum(sums[GROUP : 2 * GROUP, :], axis=0, keepdims=True), axis=1, keepdims=True)
    following = penalty * jnp.sqrt(jnp.sqrt((primal + 1.0) / (penalty * penalty * dual + 1.0)))
    return penalty, following, penalty / following


def wide(value, shape):
    return jnp.broadcast_to(value, shape)


def shrink_kernel(rows, cols, first, last, *refs):
    if first:
        fit, quad, norm, row_halo, left_halo, right_halo = refs[:6]
        outs = refs[6:]
    else:
        (fit, other, quad, norm, row_halo, left_halo, right_halo, scalars, sums) = refs[:9]
        (old_sparse, old_down, old_right, old_top, old_side) = refs[9:14]
        outs = refs[14:]
    (estimate, sparse, down_sum, right_sum, top_sum, side_sum, down_arg, right_arg, top_arg, side_arg) = outs[:10]
    residuals, new_scalars = outs[10:12]
    members = fit.shape[0]
    shape = (GROUP, cols)
    if first:
        penalty = jnp.ones((1, 1), F32)
        rescale = jnp.ones((1, 1), F32)
    else:
        before, penalty, rescale = new_penalty(scalars, sums)
        old_bound = wide(weight_tv / before, shape)
        old_sparse_bound = wide(weight_sparse / before, shape)
    new_scalars[0:1, :] = wide(penalty, (1, cols))
    new_scalars[1:2, :] = wide(rescale, (1, cols))
    bound = wide(weight_tv / penalty, shape)
    sparse_bound = wide(weight_sparse / penalty, shape)
    scale = wide(rescale, shape)
    has_above, has_below, has_left, has_right = edge_flags()
    lane = lanes_of(shape)
    keep_last = jnp.where(lane == cols - 1, has_right, 1.0)
    is_panel = jnp.where(lane < rows, has_left, 0.0)

    def mixed(a, b):
        return a + scale * b

    def shrunk(value, old, sums_now):
        primal, dual = sums_now
        if first:
            total = value
        else:
            old_total = old
            old_clip = clip(old_total, old_bound)
            total = value + scale * old_clip
        rest = total - clip(total, bound)
        arg = value - rest
        primal = primal + arg * arg
        change = rest if first else rest - (old_total - old_clip)
        dual = dual + change * change
        return total, arg, (primal, dual)

    def step(base, sums_now):
        here = pl.ds(base, GROUP)
        spans = [slice(i * cols, (i + 1) * cols) for i in range(rows)]
        if first:
            now = [fit[here, span] for span in spans]
            near_row = row_halo[here, :]
            near_left, near_right = left_halo[here, :], right_halo[here, :]
        else:
            now = [mixed(fit[here, span], other[here, span]) for span in spans]
            near_row = mixed(row_halo[here, :], row_halo[pl.ds(base + members, GROUP), :])
            near_left = mixed(left_halo[here, :], roll(left_halo[here, :], -rows))
            near_right = mixed(right_halo[here, :], roll(right_halo[here, :], -rows))
        column = jnp.zeros(shape, F32)
        for i in range(rows):
            value = now[i]
            estimate[here, spans[i]] = value
            column = jnp.where(lane == i, roll(value, i), column)
            primal, dual = sums_now
            if first:
                total = value
            else:
                old = old_sparse[here, spans[i]]
                total = value + scale * jnp.minimum(old, old_sparse_bound)
            kept = jnp.maximum(total - sparse_bound, 0.0)
            sparse[here, spans[i]] = total
            gap = value - kept
            primal = primal + gap * gap
            change = kept if first else kept - jnp.maximum(old - old_sparse_bound, 0.0)
            dual = dual + change * change
            sums_now = (primal, dual)
            if i < rows - 1:
                diff = now[i + 1] - value
            else:
                diff = (near_row - value) * has_below
            old = None if first else old_down[here, spans[i]]
            total, arg, sums_now = shrunk(diff, old, sums_now)
            down_sum[here, spans[i]] = total
            down_arg[here, spans[i]] = arg
            beside = jnp.where(lane == cols - 1, roll(near_right, cols - 1 - i), roll(value, -1))
            diff = (beside - value) * keep_last
            old = None if first else old_right[here, spans[i]]
            total, arg, sums_now = shrunk(diff, old, sums_now)
            right_sum[here, spans[i]] = total
            right_arg[here, spans[i]] = arg
        idle = (jnp.zeros(shape, F32),) * 2
        total, arg, _ = shrunk((now[0] - near_row) * has_above, None if first else old_top[here, :], idle)
        top_sum[here, :] = total
        top_arg[here, :] = arg
        panel = jnp.where(lane < rows, column - near_left, 0.0) * is_panel
        total, arg, _ = shrunk(panel, None if first else old_side[here, :], idle)
        side_sum[here, :] = total
        side_arg[here, :] = arg
        return sums_now

    zero = jnp.zeros(shape, F32)
    body, count = groups(members, step)
    primal, dual = lax.fori_loop(0, count, body, (zero, zero), unroll=UNROLL)
    total, cross, weight = quad[0:GROUP, :], quad[GROUP : 2 * GROUP, :], norm[...]
    if not first:
        total = total + scale * (quad[2 * GROUP : 3 * GROUP, :] + scale * quad[4 * GROUP : 5 * GROUP, :])
        cross = cross + scale * quad[3 * GROUP : 4 * GROUP, :]
    square = total + weight
    share = wide(1.0 / (1.0 + penalty), shape)
    part = wide(penalty / (1.0 + penalty), shape)
    if not last:
        outs[12][...] = weight + part * (2.0 * (cross - weight) + part * square)
    residuals[0:GROUP, :] = primal + share * share * square
    residuals[GROUP : 2 * GROUP, :] = dual


def sides_kernel(rows, cols, first, last, *refs):
    (estimate, sparse, down_sum, right_sum, top_sum, side_sum, down_arg, right_arg, top_arg, side_arg) = refs[:10]
    scalars, projected, fit_gram = refs[10:13]
    at = 13
    if not first:
        other_gram, old_multiplier = refs[13:15]
        at = 15
    rhs_high, rhs_low = refs[at : at + 2]
    if not last:
        side, other_side, multiplier = refs[at + 2 :]
    members = estimate.shape[0]
    shape = (GROUP, cols)
    pixels = rows * cols
    penalty, rescale = scalars[0:1, 0:1], scalars[1:2, 0:1]
    bound = wide(weight_tv / penalty, shape)
    sparse_bound = wide(weight_sparse / penalty, shape)
    scale = wide(rescale, shape)
    weight = wide(penalty, shape)
    share = wide(1.0 / (1.0 + penalty), shape)
    lane = lanes_of(shape)

    def step(base, carry):
        here = pl.ds(base, GROUP)
        arg_above, dual_above = top_arg[here, :], clip(top_sum[here, :], bound)
        arg_left, dual_left = side_arg[here, :], clip(side_sum[here, :], bound)
        for i in range(rows):
            span = slice(i * cols, (i + 1) * cols)
            later = slice(pixels + i * cols, pixels + (i + 1) * cols)
            value = estimate[here, span]
            gram = fit_gram[here, span]
            held = gram
            if not first:
                gram = gram + scale * other_gram[here, span]
                held = gram + scale * old_multiplier[here, span]
            data = (projected[here, span] + weight * held) * share
            dual_data = held - data
            down, dual_down = down_arg[here, span], clip(down_sum[here, span], bound)
            right, dual_right = right_arg[here, span], clip(right_sum[here, span], bound)
            beside = jnp.where(lane == 0, roll(arg_left, -i), roll(right, 1))
            dual_beside = jnp.where(lane == 0, roll(dual_left, -i), roll(dual_right, 1))
            total = sparse[here, span]
            rhs = data + jnp.maximum(total - sparse_bound, 0.0) + prox_tau * value - (
                (arg_above - down) + (beside - right)
            )
            rhs_other = -(
                dual_data
                + jnp.minimum(total, sparse_bound)
                + ((dual_above - dual_down) + (dual_beside - dual_right))
            )
            arg_above, dual_above = down, dual_down
            rhs_high[here, span], rhs_low[here, span] = split(rhs)
            rhs_high[here, later], rhs_low[here, later] = split(rhs_other)
            if not last:
                side[here, span] = rhs
                other_side[here, span] = rhs_other
                multiplier[here, span] = dual_data
        return carry

    body, count = groups(members, step)
    lax.fori_loop(0, count, body, 0, unroll=UNROLL)


def solve_kernel(inv_high, inv_low, rhs_high, rhs_low, fit, other):
    pixels = fit.shape[1]

    def store(start, size, value):
        if start < pixels:
            fit[:, start : start + size] = value
        else:
            other[:, start - pixels : start - pixels + size] = value

    apply_inverse(inv_high, inv_low, rhs_high, rhs_low, store)


def products_kernel(rows, cols, *refs):
    fit, other, side, other_side, multiplier, projected, scalars = refs[:7]
    fit_gram, other_gram, quad, row_edge, left_edge, right_edge = refs[7:]
    members = fit.shape[0]
    shape = (GROUP, cols)
    weight = wide(scalars[0:1, 0:1], shape)
    below = edge_flags()[1]

    def step(base, sums):
        here = pl.ds(base, GROUP)
        aa, ap, ab, bp, bb = sums
        fits, others = [], []
        for i in range(rows):
            span = slice(i * cols, (i + 1) * cols)
            a, b = fit[here, span], other[here, span]
            ga = side[here, span] - SHIFT * a
            gb = other_side[here, span] - SHIFT * b
            fit_gram[here, span] = ga
            other_gram[here, span] = gb
            target = projected[here, span] + weight * multiplier[here, span]
            aa = aa + a * (ga - 2.0 * target)
            ap = ap + a * target
            ab = ab + b * (2.0 * (ga - target))
            bp = bp + b * target
            bb = bb + b * gb
            fits.append(a)
            others.append(b)
        write_edges(base, members, fits, others, below, row_edge, left_edge, right_edge)
        return aa, ap, ab, bp, bb

    zero = jnp.zeros(shape, F32)
    body, count = groups(members, step)
    for index, value in enumerate(lax.fori_loop(0, count, body, (zero,) * 5, unroll=UNROLL)):
        quad[index * GROUP : (index + 1) * GROUP, :] = value


def finish_kernel(rows, cols, fit, other, scalars, sums, abundance):
    members = fit.shape[0]
    rescale = new_penalty(scalars, sums)[2]
    scale = wide(rescale, (members, cols))
    for i in range(rows):
        span = slice(i * cols, (i + 1) * cols)
        abundance[pl.ds(i, members, stride=rows), :] = fit[:, span] + scale * other[:, span]


def flat_swap(value, stride, other_row):
    cols = lax.axis_size("col")
    pairs = []
    for row in range(2):
        for col in range(cols):
            target = (1 - row if other_row else row) * cols + (col ^ stride)
            pairs.append((row * cols + col, target))
    return lax.ppermute(value, ("row", "col"), pairs)


def strides():
    cols = lax.axis_size("col")
    return [1 << bit for bit in reversed(range(cols.bit_length() - 1))]


def regular():
    cols = lax.axis_size("col")
    return lax.axis_size("row") == 2 and cols & (cols - 1) == 0


def total_over_mesh(value):
    if not regular():
        return lax.psum(value, ("row", "col"))
    for stride in strides() + [0]:
        value = value + flat_swap(value, stride, True)
    return value


def shifted(value, axis, step):
    count = lax.axis_size(axis)
    first, last = max(0, -step), min(count, count - step)
    return lax.ppermute(value, axis, [(source, source + step) for source in range(first, last)])


def halos(row_edge, left_edge, right_edge):
    near_row = flat_swap(row_edge, 0, True)
    near_left = shifted(right_edge, "col", 1)
    near_right = shifted(left_edge, "col", -1)
    return near_row, near_left, near_right


def gathered(library):
    half_rows = library.shape[0] // 2
    if not regular() or half_rows % 16 or lax.axis_size("col") < 2:
        return [lax.all_gather(library, "col", axis=0, tiled=True)], True
    parity = lax.axis_index("row")
    bits = lax.axis_index("col")
    for _ in strides():
        parity = parity ^ (bits & 1)
        bits = bits >> 1
    mine = lax.dynamic_slice_in_dim(library, parity * half_rows, half_rows, 0)
    tag = mine
    order = strides()
    reach = [0]
    for stride in order[:-1]:
        got = flat_swap(mine, stride, True)
        mine = jnp.concatenate([mine, got], axis=0)
        reach = reach + [r ^ stride for r in reach]
    rest = flat_swap(mine, order[-1], True)
    reach = reach + [r ^ order[-1] for r in reach]
    other = flat_swap(mine, 0, True)
    other_rest = flat_swap(rest, 0, True)
    return [mine, rest, other, other_rest, tag], reach


def iterate(observed, library):
    channels, rows, cols = observed.shape
    members = library.shape[1]
    pixels = rows * cols
    field = ((members, pixels), F32)
    strip = ((members, cols), F32)
    scalar = ((GROUP, cols), F32)
    pieces, order = gathered(library)
    flat = observed.reshape(channels, pixels)
    columns, row_edge, norm = call(
        functools.partial(survey_kernel, rows, cols),
        [((2 * rows, channels), BF16), ((channels, cols), BF16), scalar],
        [flat],
        flops=2 * rows * channels * pixels,
    )
    near = halos(row_edge, columns, columns)
    half = ((members, members), BF16)
    extended = pltpu.VMEM((members, pixels + 2 * cols), BF16)
    scratch = [
        pltpu.VMEM((members, members), F32),
        pltpu.VMEM((members, members), F32),
        extended,
        extended,
        pltpu.SMEM((2,), F32),
        pltpu.VMEM((cols, channels), BF16),
    ]
    if order is not True:
        scratch.append(pltpu.VMEM((channels, members), BF16))
    work = 2 * members * members * pixels
    projected, inv_high, inv_low, fit, fit_gram, quad, *near = call(
        functools.partial(start_kernel, rows, cols, order),
        [field, half, half, field, field, ((2 * GROUP, cols), F32), strip, strip, strip],
        [flat, *near, *pieces],
        scratch,
        flops=8 * work,
    )
    state = None
    other = other_gram = multiplier = scalars = sums = None
    for iteration in range(ITERS):
        first = iteration == 0
        last = iteration == ITERS - 1
        if first:
            args = [fit, quad, norm, *near]
        else:
            args = [fit, other, quad, norm, *near, scalars, sums, *state[1:6]]
        results = call(
            functools.partial(shrink_kernel, rows, cols, first, last),
            [field] * 4 + [strip] * 2 + [field] * 2 + [strip] * 2
            + [((2 * GROUP, cols), F32), scalar] + ([] if last else [scalar]),
            args,
            flops=work,
        )
        state, residuals, scalars = results[:10], results[10], results[11]
        sums = total_over_mesh(residuals)
        args = [*state, scalars, projected, fit_gram]
        if not first:
            args += [other_gram, multiplier]
        wide_half = ((members, 2 * pixels), BF16)
        rhs_high, rhs_low, *sides = call(
            functools.partial(sides_kernel, rows, cols, first, last),
            [wide_half] * 2 + ([] if last else [field] * 3),
            args,
            flops=2 * work,
        )
        fit, other = call(
            solve_kernel, [field] * 2, [inv_high, inv_low, rhs_high, rhs_low], flops=2 * work
        )
        if last:
            break
        multiplier = sides[2]
        fit_gram, other_gram, quad, *edge = call(
            functools.partial(products_kernel, rows, cols),
            [field] * 2 + [((5 * GROUP, cols), F32), ((2 * members, cols), F32), strip, strip],
            [fit, other, *sides, projected, scalars],
            flops=2 * work,
        )
        near = halos(*edge)
        norm = results[12]
    (abundance,) = call(
        functools.partial(finish_kernel, rows, cols),
        [((members * rows, cols), F32)],
        [fit, other, scalars, sums],
        flops=work // 8,
    )
    return abundance.reshape(members, rows, cols)


def solution(mesh):
    return jax.shard_map(
        iterate,
        mesh=mesh,
        in_specs=(P(None, "row", "col"), P("col", None)),
        out_specs=P(None, "row", "col"),
        check_vma=False,
    )
```

```python
import functools

import jax
import jax.numpy as jnp
from jax import lax
from jax.experimental import pallas as pl
from jax.experimental.pallas import tpu as pltpu
from jax.sharding import PartitionSpec as P


ITERS = 3

prox_tau = 8.0
weight_sparse = 0.3
weight_tv = 1.0

F32 = jnp.float32
BF16 = jnp.bfloat16
SHIFT = 1.0 + prox_tau
GROUP = 8
UNROLL = 16


def split(value):
    high = value.astype(BF16)
    return high, (value - high.astype(F32)).astype(BF16)


def dot(left, right):
    return jnp.dot(left, right, preferred_element_type=F32)


def dot_full(left, right):
    return jnp.dot(left, right, precision=lax.Precision.HIGHEST, preferred_element_type=F32)


def dot_columns(left, right):
    return lax.dot_general(left, right, (((0,), (0,)), ((), ())), preferred_element_type=F32)


def clip(value, bound):
    return jnp.minimum(jnp.maximum(value, -bound), bound)


def call(body, outs, args, scratch=(), flops=0, limit=24):
    return pl.pallas_call(
        body,
        out_shape=[jax.ShapeDtypeStruct(*out) for out in outs],
        in_specs=[pl.BlockSpec(memory_space=pltpu.VMEM)] * len(args),
        out_specs=[pl.BlockSpec(memory_space=pltpu.VMEM)] * len(outs),
        scratch_shapes=list(scratch),
        cost_estimate=pl.CostEstimate(flops=flops, bytes_accessed=0, transcendentals=0),
        compiler_params=pltpu.CompilerParams(vmem_limit_bytes=limit << 20),
    )(*args)


def groups(members, step):
    def body(index, carry):
        return step(pl.multiple_of(index * GROUP, GROUP), carry)

    return body, members // GROUP


def roll(value, shift):
    return pltpu.roll(value, shift % value.shape[1], 1)


def lanes_of(shape):
    return lax.broadcasted_iota(jnp.int32, shape, 1)


def flag(condition):
    return jnp.where(condition, 1.0, 0.0).astype(F32)


def edge_flags():
    row, col = lax.axis_index("row"), lax.axis_index("col")
    return (
        flag(row > 0),
        flag(row < lax.axis_size("row") - 1),
        flag(col > 0),
        flag(col < lax.axis_size("col") - 1),
    )


def invert(gram, inverse, power, left):
    eye = flag(
        lax.broadcasted_iota(jnp.int32, gram.shape, 0) == lax.broadcasted_iota(jnp.int32, gram.shape, 1)
    )
    system = gram + SHIFT * eye
    bound = jnp.max(jnp.sum(jnp.abs(gram), axis=1, keepdims=True)) + SHIFT
    nearest = jnp.sum(system * eye) / jnp.sum(system * system)
    scale = jnp.where(nearest * bound < 1.9, nearest, 2.0 / (bound + SHIFT))
    first = eye - scale * system
    squared = dot_full(first, first)
    inverse[...] = scale * (eye + first)
    power[...] = squared
    left[0] = jnp.sum(squared * squared)

    def step(index, carry):
        @pl.when(left[0] > 0.0)
        def _():
            current = power[...]
            inverse[...] = inverse[...] + dot_full(inverse[...], current)

        @pl.when(left[0] > 1e-6)
        def _():
            current = power[...]
            squared = dot_full(current, current)
            power[...] = squared
            left[1] = jnp.sum(squared * squared)

        left[0] = jnp.where(left[0] > 1e-6, left[1], 0.0)
        return carry

    lax.fori_loop(0, 20, step, 0)


def apply_inverse(inv_high, inv_low, rhs_high, rhs_low, store):
    width = rhs_high.shape[1]
    for start in range(0, width, 512):
        block = min(512, width - start)
        high, low = rhs_high[:, start : start + block], rhs_low[:, start : start + block]
        store(start, block, dot(inv_high[...], high) + (dot(inv_high[...], low) + dot(inv_low[...], high)))


def survey_kernel(rows, cols, observed, flat, columns, row_edge, norm, wide_band):
    channels, pixels = flat.shape
    tall = 2 * GROUP
    zero = jnp.zeros((tall, cols), F32)

    def widen(index, total):
        total = list(total)
        for part in range(rows):
            here = pl.ds(pl.multiple_of((index * rows + part) * tall, tall), tall)
            value = observed[here, :].astype(F32)
            wide_band[here, :] = value
            total[part % 2] = total[part % 2] + value * value
        return tuple(total)

    even, odd = lax.fori_loop(0, channels // tall, widen, (zero, zero), unroll=4)
    total = even + odd
    norm[...] = total[:GROUP, :] + total[GROUP:, :]

    def place(index, carry):
        start = pl.multiple_of(index * tall, tall)
        for i in range(rows):
            value = wide_band[pl.ds(start * rows + i, tall, stride=rows), :]
            flat[pl.ds(start, tall), i * cols : (i + 1) * cols] = value.astype(BF16)
        return carry

    lax.fori_loop(0, channels // tall, place, 0, unroll=4)
    spot = lax.broadcasted_iota(jnp.int32, (2 * rows, pixels), 0)
    pixel = lax.broadcasted_iota(jnp.int32, (2 * rows, pixels), 1)
    wanted = jnp.where(spot < rows, spot * cols, (spot - rows) * cols + cols - 1)
    chosen = flag(pixel == wanted).astype(BF16)
    columns[...] = lax.dot_general(
        chosen, flat[...], (((1,), (1,)), ((), ())), preferred_element_type=F32
    ).astype(BF16)
    is_upper = edge_flags()[1] > 0.0

    @pl.when(is_upper)
    def _():
        row_edge[...] = flat[:, pixels - cols :]

    @pl.when(jnp.logical_not(is_upper))
    def _():
        row_edge[...] = flat[:, :cols]


def start_kernel(rows, cols, order, *refs):
    ordered = order is True
    observed, row_halo, left_halo, right_halo = refs[:4]
    inputs = 5 if ordered else 9
    pieces = refs[4:inputs]
    projected, inv_high, inv_low, fit, fit_gram, quad, near_row, near_left, near_right = refs[inputs : inputs + 9]
    inverse, power, rhs_high, rhs_low, left, panel = refs[inputs + 9 : inputs + 15]
    if ordered:
        full = pieces[0]
    else:
        full = refs[inputs + 15]
        place_library(pieces, full, order)
    members = full.shape[1]
    pixels = rows * cols
    panel[...] = jnp.zeros(panel.shape, BF16)
    panel[0 : 2 * rows, :] = right_halo[...]
    panel[2 * rows : 4 * rows, :] = left_halo[...]
    block = min(512, pixels)
    for start in range(0, pixels, block):
        span = slice(start, start + block)
        result = dot_columns(full[...], observed[:, span])
        projected[:, span] = result
        rhs_high[:, span], rhs_low[:, span] = split(result)
    span = slice(pixels, pixels + cols)
    rhs_high[:, span], rhs_low[:, span] = split(dot_columns(full[...], row_halo[...]))
    span = slice(pixels + cols, pixels + cols + panel.shape[0])
    beside = lax.dot_general(full[...], panel[...], (((0,), (1,)), ((), ())), preferred_element_type=F32)
    rhs_high[:, span], rhs_low[:, span] = split(beside)
    invert(dot_columns(full[...], full[...]), inverse, power, left)
    inv_high[...], inv_low[...] = split(inverse[...])

    def store(start, size, value):
        if start < pixels:
            fit[:, start : start + size] = value
        else:
            near_row[...] = value[:, :cols]
            near_right[...] = value[:, cols:]
            near_left[...] = roll(value[:, cols:], -3 * rows)

    apply_inverse(inv_high, inv_low, rhs_high, rhs_low, store)

    def step(base, sums):
        here = pl.ds(base, GROUP)
        total, cross = sums
        for i in range(rows):
            span = slice(i * cols, (i + 1) * cols)
            a, p = fit[here, span], projected[here, span]
            ga = p - SHIFT * a
            fit_gram[here, span] = ga
            total = total + a * (ga - 2.0 * p)
            cross = cross + a * p
        return total, cross

    zero = jnp.zeros((GROUP, cols), F32)
    body, count = groups(members, step)
    total, cross = lax.fori_loop(0, count, body, (zero, zero), unroll=UNROLL)
    quad[0:GROUP, :] = total
    quad[GROUP : 2 * GROUP, :] = cross


def write_edges(base, members, a, b, below, row_edge, panel):
    here = pl.ds(base, GROUP)
    is_upper = below > 0.0
    row_edge[here, :] = jnp.where(is_upper, a[-1], a[0])
    row_edge[pl.ds(base + members, GROUP), :] = jnp.where(is_upper, b[-1], b[0])
    lane = lanes_of(a[0].shape)
    cols = a[0].shape[1]
    count = len(a) + len(b)
    first = jnp.zeros_like(a[0])
    final = jnp.zeros_like(a[0])
    for i, value in enumerate(a + b):
        turned = roll(value, i)
        first = jnp.where(lane == i, turned, first)
        final = jnp.where(lane == (i - 1) % cols, turned, final)
    panel[here, :] = jnp.where(lane < count, first, roll(final, count + 1))


def pack_edges(panel, rows, to_pair, to_next):
    members, cols = panel.shape
    count = 2 * rows
    is_odd = (lax.axis_index("col") & 1) > 0
    for part in range(members // cols):
        turned = jnp.transpose(panel[part * cols : (part + 1) * cols, :])
        first, final = turned[:count, :], turned[count : 2 * count, :]
        here = slice(part * count, (part + 1) * count)
        to_pair[here, :] = jnp.where(is_odd, first, final)
        to_next[here, :] = jnp.where(is_odd, final, first)


def unpack_edges(panel, rows, from_pair, skip, from_next):
    members, cols = panel.shape
    count = 2 * rows
    is_odd = (lax.axis_index("col") & 1) > 0
    rest = jnp.zeros((cols - 2 * count, cols), F32)
    for part in range(members // cols):
        pair = from_pair[skip + part * count : skip + (part + 1) * count, :]
        other = from_next[part * count : (part + 1) * count, :]
        on_left, on_right = jnp.where(is_odd, pair, other), jnp.where(is_odd, other, pair)
        panel[part * cols : (part + 1) * cols, :] = jnp.transpose(
            jnp.concatenate([on_left, on_right, rest], axis=0)
        )


def place_library(pieces, full, order):
    mine, mine_rest, other, other_rest, rows_of = pieces
    rows = rows_of.shape[0]
    own = lax.axis_index("col")
    parity = lax.axis_index("row")
    bits = own
    for _ in range(max(1, (lax.axis_size("col") - 1).bit_length())):
        parity = parity ^ (bits & 1)
        bits = bits >> 1
    half = parity
    blocks = mine.shape[0] // rows
    for offset, first, second in ((0, mine, other), (blocks, mine_rest, other_rest)):
        for block in range(blocks):
            base = (own ^ order[block + offset]) * (2 * rows)
            source = slice(block * rows, (block + 1) * rows)
            full[pl.ds(pl.multiple_of(base + half * rows, rows), rows), :] = first[source, :]
            full[pl.ds(pl.multiple_of(base + (1 - half) * rows, rows), rows), :] = second[source, :]


def new_penalty(scalars, sums):
    penalty = scalars[0:1, 0:1]
    primal = jnp.sum(jnp.sum(sums[0:GROUP, :], axis=0, keepdims=True), axis=1, keepdims=True)
    dual = jnp.sum(jnp.sum(sums[GROUP : 2 * GROUP, :], axis=0, keepdims=True), axis=1, keepdims=True)
    following = penalty * jnp.sqrt(jnp.sqrt((primal + 1.0) / (penalty * penalty * dual + 1.0)))
    return penalty, following, penalty / following


def wide(value, shape):
    return jnp.broadcast_to(value, shape)


def shrink_kernel(rows, cols, first, last, *refs):
    if first:
        fit, quad, norm, row_halo, left_halo, right_halo = refs[:6]
        outs = refs[6:]
    else:
        (fit, other, quad, norm, row_halo, from_pair, from_next, scalars, sums) = refs[:9]
        (old_sparse, old_down, old_right, old_top, old_side) = refs[9:14]
        outs = refs[14:]
        beside = outs[-1]
        unpack_edges(beside, rows, from_pair, 2 * GROUP, from_next)
    (estimate, sparse, down_sum, right_sum, top_sum, side_sum, down_arg, right_arg, top_arg, side_arg) = outs[:10]
    residuals, new_scalars = outs[10:12]
    members = fit.shape[0]
    shape = (GROUP, cols)
    if first:
        penalty = jnp.ones((1, 1), F32)
        rescale = jnp.ones((1, 1), F32)
    else:
        before, penalty, rescale = new_penalty(scalars, sums)
        old_bound = wide(weight_tv / before, shape)
        old_sparse_bound = wide(weight_sparse / before, shape)
    new_scalars[0:1, :] = wide(penalty, (1, cols))
    new_scalars[1:2, :] = wide(rescale, (1, cols))
    bound = wide(weight_tv / penalty, shape)
    sparse_bound = wide(weight_sparse / penalty, shape)
    scale = wide(rescale, shape)
    has_above, has_below, has_left, has_right = edge_flags()
    lane = lanes_of(shape)
    keep_last = jnp.where(lane == cols - 1, has_right, 1.0)
    is_panel = jnp.where(lane < rows, has_left, 0.0)

    def mixed(a, b):
        return a + scale * b

    def shrunk(value, old, sums_now):
        primal, dual = sums_now
        if first:
            total = value
        else:
            old_total = old
            old_clip = clip(old_total, old_bound)
            total = value + scale * old_clip
        rest = total - clip(total, bound)
        arg = value - rest
        primal = primal + arg * arg
        change = rest if first else rest - (old_total - old_clip)
        dual = dual + change * change
        return total, arg, (primal, dual)

    def step(base, sums_now):
        here = pl.ds(base, GROUP)
        spans = [slice(i * cols, (i + 1) * cols) for i in range(rows)]
        if first:
            now = [fit[here, span] for span in spans]
            near_row = row_halo[here, :]
            near_left, near_right = left_halo[here, :], right_halo[here, :]
        else:
            now = [mixed(fit[here, span], other[here, span]) for span in spans]
            near_row = mixed(row_halo[here, :], row_halo[pl.ds(base + members, GROUP), :])
            near_left = mixed(beside[here, :], roll(beside[here, :], -rows))
            near_right = roll(near_left, -2 * rows)
        column = jnp.zeros(shape, F32)
        for i in range(rows):
            value = now[i]
            estimate[here, spans[i]] = value
            column = jnp.where(lane == i, roll(value, i), column)
            primal, dual = sums_now
            if first:
                total = value
            else:
                old = old_sparse[here, spans[i]]
                total = value + scale * jnp.minimum(old, old_sparse_bound)
            kept = jnp.maximum(total - sparse_bound, 0.0)
            sparse[here, spans[i]] = total
            gap = value - kept
            primal = primal + gap * gap
            change = kept if first else kept - jnp.maximum(old - old_sparse_bound, 0.0)
            dual = dual + change * change
            sums_now = (primal, dual)
            if i < rows - 1:
                diff = now[i + 1] - value
            else:
                diff = (near_row - value) * has_below
            old = None if first else old_down[here, spans[i]]
            total, arg, sums_now = shrunk(diff, old, sums_now)
            down_sum[here, spans[i]] = total
            down_arg[here, spans[i]] = arg
            following = jnp.where(lane == cols - 1, roll(near_right, cols - 1 - i), roll(value, -1))
            diff = (following - value) * keep_last
            old = None if first else old_right[here, spans[i]]
            total, arg, sums_now = shrunk(diff, old, sums_now)
            right_sum[here, spans[i]] = total
            right_arg[here, spans[i]] = arg
        idle = (jnp.zeros(shape, F32),) * 2
        total, arg, _ = shrunk((now[0] - near_row) * has_above, None if first else old_top[here, :], idle)
        top_sum[here, :] = total
        top_arg[here, :] = arg
        panel = jnp.where(lane < rows, column - near_left, 0.0) * is_panel
        total, arg, _ = shrunk(panel, None if first else old_side[here, :], idle)
        side_sum[here, :] = total
        side_arg[here, :] = arg
        return sums_now

    zero = jnp.zeros(shape, F32)
    body, count = groups(members, step)
    primal, dual = lax.fori_loop(0, count, body, (zero, zero), unroll=UNROLL)
    total, cross, weight = quad[0:GROUP, :], quad[GROUP : 2 * GROUP, :], norm[...]
    if not first:
        total = total + scale * (quad[2 * GROUP : 3 * GROUP, :] + scale * quad[4 * GROUP : 5 * GROUP, :])
        cross = cross + scale * quad[3 * GROUP : 4 * GROUP, :]
    square = total + weight
    share = wide(1.0 / (1.0 + penalty), shape)
    part = wide(penalty / (1.0 + penalty), shape)
    if not last:
        outs[12][...] = weight + part * (2.0 * (cross - weight) + part * square)
    residuals[0:GROUP, :] = primal + share * share * square
    residuals[GROUP : 2 * GROUP, :] = dual


def sides_kernel(rows, cols, first, last, *refs):
    (estimate, sparse, down_sum, right_sum, top_sum, side_sum, down_arg, right_arg, top_arg, side_arg) = refs[:10]
    scalars, projected, fit_gram = refs[10:13]
    at = 13
    if not first:
        other_gram, old_multiplier = refs[13:15]
        at = 15
    rhs_high, rhs_low = refs[at : at + 2]
    if not last:
        side, other_side, multiplier = refs[at + 2 :]
    members = estimate.shape[0]
    shape = (GROUP, cols)
    pixels = rows * cols
    penalty, rescale = scalars[0:1, 0:1], scalars[1:2, 0:1]
    bound = wide(weight_tv / penalty, shape)
    sparse_bound = wide(weight_sparse / penalty, shape)
    scale = wide(rescale, shape)
    weight = wide(penalty, shape)
    share = wide(1.0 / (1.0 + penalty), shape)
    lane = lanes_of(shape)

    def step(base, carry):
        here = pl.ds(base, GROUP)
        arg_above, dual_above = top_arg[here, :], clip(top_sum[here, :], bound)
        arg_left, dual_left = side_arg[here, :], clip(side_sum[here, :], bound)
        for i in range(rows):
            span = slice(i * cols, (i + 1) * cols)
            later = slice(pixels + i * cols, pixels + (i + 1) * cols)
            value = estimate[here, span]
            gram = fit_gram[here, span]
            held = gram
            if not first:
                gram = gram + scale * other_gram[here, span]
                held = gram + scale * old_multiplier[here, span]
            data = (projected[here, span] + weight * held) * share
            dual_data = held - data
            down, dual_down = down_arg[here, span], clip(down_sum[here, span], bound)
            right, dual_right = right_arg[here, span], clip(right_sum[here, span], bound)
            beside = jnp.where(lane == 0, roll(arg_left, -i), roll(right, 1))
            dual_beside = jnp.where(lane == 0, roll(dual_left, -i), roll(dual_right, 1))
            total = sparse[here, span]
            rhs = data + jnp.maximum(total - sparse_bound, 0.0) + prox_tau * value - (
                (arg_above - down) + (beside - right)
            )
            rhs_other = -(
                dual_data
                + jnp.minimum(total, sparse_bound)
                + ((dual_above - dual_down) + (dual_beside - dual_right))
            )
            arg_above, dual_above = down, dual_down
            rhs_high[here, span], rhs_low[here, span] = split(rhs)
            rhs_high[here, later], rhs_low[here, later] = split(rhs_other)
            if not last:
                side[here, span] = rhs
                other_side[here, span] = rhs_other
                multiplier[here, span] = dual_data
        return carry

    body, count = groups(members, step)
    lax.fori_loop(0, count, body, 0, unroll=UNROLL)


def solve_kernel(rows, cols, last, *refs):
    inv_high, inv_low, rhs_high, rhs_low = refs[:4]
    if last:
        fit, other = refs[4:]
    else:
        side, other_side, multiplier, projected, scalars = refs[4:9]
        fit, other, fit_gram, other_gram, quad, row_edge, to_pair, to_next, panel = refs[9:]
    members, pixels = fit.shape

    def store(start, size, value):
        if start < pixels:
            fit[:, start : start + size] = value
        else:
            other[:, start - pixels : start - pixels + size] = value

    apply_inverse(inv_high, inv_low, rhs_high, rhs_low, store)
    if last:
        return
    shape = (GROUP, cols)
    weight = wide(scalars[0:1, 0:1], shape)
    below = edge_flags()[1]

    def step(base, sums):
        here = pl.ds(base, GROUP)
        aa, ap, ab, bp, bb = sums
        fits, others = [], []
        for i in range(rows):
            span = slice(i * cols, (i + 1) * cols)
            a, b = fit[here, span], other[here, span]
            ga = side[here, span] - SHIFT * a
            gb = other_side[here, span] - SHIFT * b
            fit_gram[here, span] = ga
            other_gram[here, span] = gb
            target = projected[here, span] + weight * multiplier[here, span]
            aa = aa + a * (ga - 2.0 * target)
            ap = ap + a * target
            ab = ab + b * (2.0 * (ga - target))
            bp = bp + b * target
            bb = bb + b * gb
            fits.append(a)
            others.append(b)
        write_edges(base, members, fits, others, below, row_edge, panel)
        return aa, ap, ab, bp, bb

    zero = jnp.zeros(shape, F32)
    body, count = groups(members, step)
    for index, value in enumerate(lax.fori_loop(0, count, body, (zero,) * 5, unroll=UNROLL)):
        quad[index * GROUP : (index + 1) * GROUP, :] = value
    pack_edges(panel, rows, to_pair, to_next)


def finish_kernel(rows, cols, fit, other, scalars, sums, abundance):
    members = fit.shape[0]
    rescale = new_penalty(scalars, sums)[2]
    scale = wide(rescale, (members, cols))
    for i in range(rows):
        span = slice(i * cols, (i + 1) * cols)
        abundance[pl.ds(i, members, stride=rows), :] = fit[:, span] + scale * other[:, span]


def flat_swap(value, stride, other_row):
    cols = lax.axis_size("col")
    pairs = []
    for row in range(2):
        for col in range(cols):
            target = (1 - row if other_row else row) * cols + (col ^ stride)
            pairs.append((row * cols + col, target))
    return lax.ppermute(value, ("row", "col"), pairs)


def strides():
    cols = lax.axis_size("col")
    return [1 << bit for bit in reversed(range(cols.bit_length() - 1))]


def regular():
    cols = lax.axis_size("col")
    return lax.axis_size("row") == 2 and cols & (cols - 1) == 0


def total_over_mesh(value):
    if not regular():
        return lax.psum(value, ("row", "col"))
    for stride in strides() + [0]:
        value = value + flat_swap(value, stride, True)
    return value


def shifted(value, axis, step):
    count = lax.axis_size(axis)
    first, last = max(0, -step), min(count, count - step)
    return lax.ppermute(value, axis, [(source, source + step) for source in range(first, last)])


def band_halos(row_edge, columns):
    near_row = flat_swap(row_edge, 0, True)
    near_left = shifted(columns, "col", 1)
    near_right = shifted(columns, "col", -1)
    return near_row, near_left, near_right


def next_swap(value):
    count = lax.axis_size("col")
    pairs = []
    for low in range(1, count - 1, 2):
        pairs += [(low, low + 1), (low + 1, low)]
    return lax.ppermute(value, "col", pairs)


def sums_and_halos(value, edges):
    row_edge, to_pair, to_next = edges
    near_row = flat_swap(row_edge, 0, True)
    from_next = next_swap(to_next)
    if not regular():
        both = jnp.concatenate([value, to_pair], axis=0)
        pairs = [(c, c ^ 1) for c in range(lax.axis_size("col")) if c ^ 1 < lax.axis_size("col")]
        return lax.psum(value, ("row", "col")), near_row, lax.ppermute(both, "col", pairs), from_next
    stages = strides()
    for stride in stages[:-1]:
        value = value + flat_swap(value, stride, True)
    from_pair = flat_swap(jnp.concatenate([value, to_pair], axis=0), stages[-1], False)
    value = value + from_pair[: value.shape[0], :]
    value = value + flat_swap(value, 0, True)
    return value, near_row, from_pair, from_next


def gathered(library):
    half_rows = library.shape[0] // 2
    if not regular() or half_rows % 16 or lax.axis_size("col") < 2:
        return [lax.all_gather(library, "col", axis=0, tiled=True)], True
    parity = lax.axis_index("row")
    bits = lax.axis_index("col")
    for _ in strides():
        parity = parity ^ (bits & 1)
        bits = bits >> 1
    mine = lax.dynamic_slice_in_dim(library, parity * half_rows, half_rows, 0)
    tag = mine
    order = strides()
    reach = [0]
    for stride in order[:-1]:
        got = flat_swap(mine, stride, True)
        mine = jnp.concatenate([mine, got], axis=0)
        reach = reach + [r ^ stride for r in reach]
    rest = flat_swap(mine, order[-1], True)
    reach = reach + [r ^ order[-1] for r in reach]
    other = flat_swap(mine, 0, True)
    other_rest = flat_swap(rest, 0, True)
    return [mine, rest, other, other_rest, tag], reach


def iterate(observed, library):
    channels, rows, cols = observed.shape
    members = library.shape[1]
    pixels = rows * cols
    field = ((members, pixels), F32)
    strip = ((members, cols), F32)
    scalar = ((GROUP, cols), F32)
    pieces, order = gathered(library)
    flat, columns, row_edge, norm = call(
        functools.partial(survey_kernel, rows, cols),
        [((channels, pixels), BF16), ((2 * rows, channels), BF16), ((channels, cols), BF16), scalar],
        [observed.reshape(channels * rows, cols)],
        [pltpu.VMEM((channels * rows, cols), F32)],
        flops=2 * rows * channels * pixels,
    )
    near = band_halos(row_edge, columns)
    half = ((members, members), BF16)
    extended = pltpu.VMEM((members, pixels + 2 * cols), BF16)
    scratch = [
        pltpu.VMEM((members, members), F32),
        pltpu.VMEM((members, members), F32),
        extended,
        extended,
        pltpu.SMEM((2,), F32),
        pltpu.VMEM((cols, channels), BF16),
    ]
    if order is not True:
        scratch.append(pltpu.VMEM((channels, members), BF16))
    work = 2 * members * members * pixels
    projected, inv_high, inv_low, fit, fit_gram, quad, *near = call(
        functools.partial(start_kernel, rows, cols, order),
        [field, half, half, field, field, ((2 * GROUP, cols), F32), strip, strip, strip],
        [flat, *near, *pieces],
        scratch,
        flops=8 * work,
    )
    state = None
    other = other_gram = multiplier = scalars = sums = None
    for iteration in range(ITERS):
        first = iteration == 0
        last = iteration == ITERS - 1
        if first:
            args = [fit, quad, norm, *near]
        else:
            args = [fit, other, quad, norm, *near, scalars, sums, *state[1:6]]
        results = call(
            functools.partial(shrink_kernel, rows, cols, first, last),
            [field] * 4 + [strip] * 2 + [field] * 2 + [strip] * 2
            + [((2 * GROUP, cols), F32), scalar] + ([] if last else [scalar]),
            args,
            [] if first else [pltpu.VMEM(*strip)],
            flops=work,
        )
        state, residuals, scalars = results[:10], results[10], results[11]
        if last:
            sums = total_over_mesh(residuals)
        args = [*state, scalars, projected, fit_gram]
        if not first:
            args += [other_gram, multiplier]
        wide_half = ((members, 2 * pixels), BF16)
        rhs_high, rhs_low, *sides = call(
            functools.partial(sides_kernel, rows, cols, first, last),
            [wide_half] * 2 + ([] if last else [field] * 3),
            args,
            flops=2 * work,
        )
        packed = ((2 * rows * members // cols, cols), F32)
        if last:
            outs, more = [], []
        else:
            multiplier = sides[2]
            outs = [field] * 2 + [((5 * GROUP, cols), F32), ((2 * members, cols), F32), packed, packed]
            more = [*sides, projected, scalars]
        results_of = call(
            functools.partial(solve_kernel, rows, cols, last),
            [field] * 2 + outs,
            [inv_high, inv_low, rhs_high, rhs_low, *more],
            [] if last else [pltpu.VMEM(*strip)],
            flops=2 * work,
        )
        fit, other = results_of[:2]
        if last:
            break
        fit_gram, other_gram, quad, *edge = results_of[2:]
        sums, *near = sums_and_halos(residuals, edge)
        norm = results[12]
    (abundance,) = call(
        functools.partial(finish_kernel, rows, cols),
        [((members * rows, cols), F32)],
        [fit, other, scalars, sums],
        flops=work // 8,
    )
    return abundance.reshape(members, rows, cols)


def solution(mesh):
    return jax.shard_map(
        iterate,
        mesh=mesh,
        in_specs=(P(None, "row", "col"), P("col", None)),
        out_specs=P(None, "row", "col"),
        check_vma=False,
    )
```

```python
import functools

import jax
import jax.numpy as jnp
from jax import lax
from jax.experimental import pallas as pl
from jax.experimental.pallas import tpu as pltpu
from jax.sharding import PartitionSpec as P


ITERS = 3

prox_tau = 8.0
weight_sparse = 0.3
weight_tv = 1.0

F32 = jnp.float32
BF16 = jnp.bfloat16
SHIFT = 1.0 + prox_tau
GROUP = 8
UNROLL = 16


def split(value):
    high = value.astype(BF16)
    return high, (value - high.astype(F32)).astype(BF16)


def dot(left, right):
    return jnp.dot(left, right, preferred_element_type=F32)


def dot_full(left, right):
    return jnp.dot(left, right, precision=lax.Precision.HIGHEST, preferred_element_type=F32)


def dot_columns(left, right):
    return lax.dot_general(left, right, (((0,), (0,)), ((), ())), preferred_element_type=F32)


def clip(value, bound):
    return jnp.minimum(jnp.maximum(value, -bound), bound)


def call(body, outs, args, scratch=(), flops=0, limit=24, space=pltpu.VMEM):
    return pl.pallas_call(
        body,
        out_shape=[jax.ShapeDtypeStruct(*out) for out in outs],
        in_specs=[pl.BlockSpec(memory_space=space)] * len(args),
        out_specs=[pl.BlockSpec(memory_space=pltpu.VMEM)] * len(outs),
        scratch_shapes=list(scratch),
        cost_estimate=pl.CostEstimate(flops=flops, bytes_accessed=0, transcendentals=0),
        compiler_params=pltpu.CompilerParams(vmem_limit_bytes=limit << 20),
    )(*args)


def groups(members, step):
    def body(index, carry):
        return step(pl.multiple_of(index * GROUP, GROUP), carry)

    return body, members // GROUP


def roll(value, shift):
    return pltpu.roll(value, shift % value.shape[1], 1)


def lanes_of(shape):
    return lax.broadcasted_iota(jnp.int32, shape, 1)


def flag(condition):
    return jnp.where(condition, 1.0, 0.0).astype(F32)


def edge_flags():
    row, col = lax.axis_index("row"), lax.axis_index("col")
    return (
        flag(row > 0),
        flag(row < lax.axis_size("row") - 1),
        flag(col > 0),
        flag(col < lax.axis_size("col") - 1),
    )


def invert(gram, inverse, power, left):
    eye = flag(
        lax.broadcasted_iota(jnp.int32, gram.shape, 0) == lax.broadcasted_iota(jnp.int32, gram.shape, 1)
    )
    system = gram + SHIFT * eye
    bound = jnp.max(jnp.sum(jnp.abs(gram), axis=1, keepdims=True)) + SHIFT
    nearest = jnp.sum(system * eye) / jnp.sum(system * system)
    scale = jnp.where(nearest * bound < 1.9, nearest, 2.0 / (bound + SHIFT))
    first = eye - scale * system
    squared = dot_full(first, first)
    inverse[...] = scale * (eye + first)
    power[...] = squared
    left[0] = jnp.sum(squared * squared)

    def step(index, carry):
        @pl.when(left[0] > 0.0)
        def _():
            current = power[...]
            inverse[...] = inverse[...] + dot_full(inverse[...], current)

        @pl.when(left[0] > 1e-6)
        def _():
            current = power[...]
            squared = dot_full(current, current)
            power[...] = squared
            left[1] = jnp.sum(squared * squared)

        left[0] = jnp.where(left[0] > 1e-6, left[1], 0.0)
        return carry

    lax.fori_loop(0, 20, step, 0)


def apply_inverse(inv_high, inv_low, rhs_high, rhs_low, store):
    width = rhs_high.shape[1]
    for start in range(0, width, 512):
        block = min(512, width - start)
        high, low = rhs_high[:, start : start + block], rhs_low[:, start : start + block]
        store(start, block, dot(inv_high[...], high) + (dot(inv_high[...], low) + dot(inv_low[...], high)))


def survey_kernel(rows, cols, observed, flat, columns, row_edge, norm, band, wide_band, arrived):
    channels, pixels = flat.shape
    tall = 2 * GROUP
    zero = jnp.zeros((tall, cols), F32)
    parts = arrived.shape[0]
    size = channels * rows // parts
    copies = []
    for part in range(parts):
        here = pl.ds(part * size, size)
        copies.append(pltpu.make_async_copy(observed.at[here, :], band.at[here, :], arrived.at[part]))
        copies[-1].start()

    def widen(index, total):
        total = list(total)
        for part in range(rows):
            here = pl.ds(pl.multiple_of((index * rows + part) * tall, tall), tall)
            value = band[here, :].astype(F32)
            wide_band[here, :] = value
            total[part % 2] = total[part % 2] + value * value
        return tuple(total)

    total = (zero, zero)
    steps = channels // tall // parts
    for part in range(parts):
        copies[part].wait()
        total = lax.fori_loop(part * steps, (part + 1) * steps, widen, total, unroll=4)
    total = total[0] + total[1]
    norm[...] = total[:GROUP, :] + total[GROUP:, :]

    def place(index, carry):
        start = pl.multiple_of(index * tall, tall)
        for i in range(rows):
            value = wide_band[pl.ds(start * rows + i, tall, stride=rows), :]
            flat[pl.ds(start, tall), i * cols : (i + 1) * cols] = value.astype(BF16)
        return carry

    lax.fori_loop(0, channels // tall, place, 0, unroll=4)
    spot = lax.broadcasted_iota(jnp.int32, (2 * rows, pixels), 0)
    pixel = lax.broadcasted_iota(jnp.int32, (2 * rows, pixels), 1)
    wanted = jnp.where(spot < rows, spot * cols, (spot - rows) * cols + cols - 1)
    chosen = flag(pixel == wanted).astype(BF16)
    columns[...] = lax.dot_general(
        chosen, flat[...], (((1,), (1,)), ((), ())), preferred_element_type=F32
    ).astype(BF16)
    is_upper = edge_flags()[1] > 0.0

    @pl.when(is_upper)
    def _():
        row_edge[...] = flat[:, pixels - cols :]

    @pl.when(jnp.logical_not(is_upper))
    def _():
        row_edge[...] = flat[:, :cols]


def gather_half(observed, first_half, second_half, order, half, library_part, band_part):
    blocks = len(order)
    rows = first_half.shape[0] // blocks
    own = lax.axis_index("col")
    for block in range(blocks):
        at = block * 2 * rows
        source = slice(block * rows, (block + 1) * rows)
        library_part[pl.ds(pl.multiple_of(at + half * rows, rows), rows), :] = first_half[source, :]
        library_part[pl.ds(pl.multiple_of(at + (1 - half) * rows, rows), rows), :] = second_half[source, :]
        base = pl.multiple_of((own ^ order[block]) * (2 * rows), 2 * rows)
        band_part[at : at + 2 * rows, :] = observed[pl.ds(base, 2 * rows), :]


def own_half():
    parity = lax.axis_index("row")
    bits = lax.axis_index("col")
    for _ in range(max(1, (lax.axis_size("col") - 1).bit_length())):
        parity = parity ^ (bits & 1)
        bits = bits >> 1
    return parity


def early_kernel(order, observed, mine, other, projected, gram, library_part, band_part):
    gather_half(observed, mine, other, order, own_half(), library_part, band_part)
    pixels = band_part.shape[1]
    for start in range(0, pixels, 512):
        span = slice(start, min(start + 512, pixels))
        projected[:, span] = dot_columns(library_part[...], band_part[:, span])
    gram[...] = dot_columns(library_part[...], library_part[...])


def start_kernel(rows, cols, order, *refs):
    ordered = order is True
    observed, row_halo, from_pair, from_next = refs[:4]
    inputs = 5 if ordered else 11
    pieces = refs[4:inputs]
    projected, inv_high, inv_low, fit, fit_gram, quad, near_row, near_left, near_right = refs[inputs : inputs + 9]
    inverse, power, rhs_high, rhs_low, left, panel = refs[inputs + 9 : inputs + 15]
    if ordered:
        full = pieces[0]
    else:
        full, library_part, band_part = refs[inputs + 15 :]
        place_library(pieces[:5], full, order)
        early, early_gram = pieces[5:]
        late = order[len(order) // 2 :]
        gather_half(observed, pieces[1], pieces[3], late, own_half(), library_part, band_part)
    members = full.shape[1]
    pixels = rows * cols
    panel[...] = jnp.zeros(panel.shape, BF16)
    is_odd = (lax.axis_index("col") & 1) > 0
    for low, odd_one, even_one in ((0, from_next, from_pair), (2 * rows, from_pair, from_next)):

        @pl.when(is_odd)
        def _():
            panel[low : low + 2 * rows, :] = odd_one[...]

        @pl.when(jnp.logical_not(is_odd))
        def _():
            panel[low : low + 2 * rows, :] = even_one[...]

    block = min(512, pixels)
    for start in range(0, pixels, block):
        span = slice(start, start + block)
        if ordered:
            result = dot_columns(full[...], observed[:, span])
        else:
            result = early[:, span] + dot_columns(library_part[...], band_part[:, span])
        projected[:, span] = result
        rhs_high[:, span], rhs_low[:, span] = split(result)
    span = slice(pixels, pixels + cols)
    rhs_high[:, span], rhs_low[:, span] = split(dot_columns(full[...], row_halo[...]))
    span = slice(pixels + cols, pixels + cols + panel.shape[0])
    beside = lax.dot_general(full[...], panel[...], (((0,), (1,)), ((), ())), preferred_element_type=F32)
    rhs_high[:, span], rhs_low[:, span] = split(beside)
    if ordered:
        gram = dot_columns(full[...], full[...])
    else:
        gram = early_gram[...] + dot_columns(library_part[...], library_part[...])
    invert(gram, inverse, power, left)
    inv_high[...], inv_low[...] = split(inverse[...])

    def store(start, size, value):
        if start < pixels:
            fit[:, start : start + size] = value
        else:
            near_row[...] = value[:, :cols]
            near_right[...] = value[:, cols:]
            near_left[...] = roll(value[:, cols:], -3 * rows)

    apply_inverse(inv_high, inv_low, rhs_high, rhs_low, store)

    def step(base, sums):
        here = pl.ds(base, GROUP)
        total, cross = sums
        for i in range(rows):
            span = slice(i * cols, (i + 1) * cols)
            a, p = fit[here, span], projected[here, span]
            ga = p - SHIFT * a
            fit_gram[here, span] = ga
            total = total + a * (ga - 2.0 * p)
            cross = cross + a * p
        return total, cross

    zero = jnp.zeros((GROUP, cols), F32)
    body, count = groups(members, step)
    total, cross = lax.fori_loop(0, count, body, (zero, zero), unroll=UNROLL)
    quad[0:GROUP, :] = total
    quad[GROUP : 2 * GROUP, :] = cross


def write_edges(base, members, a, b, below, row_edge, panel):
    here = pl.ds(base, GROUP)
    is_upper = below > 0.0
    row_edge[here, :] = jnp.where(is_upper, a[-1], a[0])
    row_edge[pl.ds(base + members, GROUP), :] = jnp.where(is_upper, b[-1], b[0])
    lane = lanes_of(a[0].shape)
    cols = a[0].shape[1]
    count = len(a) + len(b)
    first = jnp.zeros_like(a[0])
    final = jnp.zeros_like(a[0])
    for i, value in enumerate(a + b):
        turned = roll(value, i)
        first = jnp.where(lane == i, turned, first)
        final = jnp.where(lane == (i - 1) % cols, turned, final)
    panel[here, :] = jnp.where(lane < count, first, roll(final, count + 1))


def pack_edges(panel, rows, to_pair, to_next):
    members, cols = panel.shape
    count = 2 * rows
    is_odd = (lax.axis_index("col") & 1) > 0
    for part in range(members // cols):
        turned = jnp.transpose(panel[part * cols : (part + 1) * cols, :])
        first, final = turned[:count, :], turned[count : 2 * count, :]
        here = slice(part * count, (part + 1) * count)
        to_pair[here, :] = jnp.where(is_odd, first, final)
        to_next[here, :] = jnp.where(is_odd, final, first)


def unpack_edges(panel, rows, from_pair, skip, from_next):
    members, cols = panel.shape
    count = 2 * rows
    is_odd = (lax.axis_index("col") & 1) > 0
    rest = jnp.zeros((cols - 2 * count, cols), F32)
    for part in range(members // cols):
        pair = from_pair[skip + part * count : skip + (part + 1) * count, :]
        other = from_next[part * count : (part + 1) * count, :]
        on_left, on_right = jnp.where(is_odd, pair, other), jnp.where(is_odd, other, pair)
        panel[part * cols : (part + 1) * cols, :] = jnp.transpose(
            jnp.concatenate([on_left, on_right, rest], axis=0)
        )


def place_library(pieces, full, order):
    mine, mine_rest, other, other_rest, rows_of = pieces
    rows = rows_of.shape[0]
    own = lax.axis_index("col")
    parity = lax.axis_index("row")
    bits = own
    for _ in range(max(1, (lax.axis_size("col") - 1).bit_length())):
        parity = parity ^ (bits & 1)
        bits = bits >> 1
    half = parity
    blocks = mine.shape[0] // rows
    for offset, first, second in ((0, mine, other), (blocks, mine_rest, other_rest)):
        for block in range(blocks):
            base = (own ^ order[block + offset]) * (2 * rows)
            source = slice(block * rows, (block + 1) * rows)
            full[pl.ds(pl.multiple_of(base + half * rows, rows), rows), :] = first[source, :]
            full[pl.ds(pl.multiple_of(base + (1 - half) * rows, rows), rows), :] = second[source, :]


def new_penalty(scalars, sums):
    penalty = scalars[0:1, 0:1]
    primal = jnp.sum(jnp.sum(sums[0:GROUP, :], axis=0, keepdims=True), axis=1, keepdims=True)
    dual = jnp.sum(jnp.sum(sums[GROUP : 2 * GROUP, :], axis=0, keepdims=True), axis=1, keepdims=True)
    following = penalty * jnp.sqrt(jnp.sqrt((primal + 1.0) / (penalty * penalty * dual + 1.0)))
    return penalty, following, penalty / following


def wide(value, shape):
    return jnp.broadcast_to(value, shape)


def shrink_kernel(rows, cols, first, last, *refs):
    if first:
        fit, quad, norm, row_halo, left_halo, right_halo = refs[:6]
        outs = refs[6:]
    else:
        (fit, other, quad, norm, row_halo, from_pair, from_next, scalars, sums) = refs[:9]
        (old_sparse, old_down, old_right, old_top, old_side) = refs[9:14]
        outs = refs[14:]
        beside = outs[-1]
        unpack_edges(beside, rows, from_pair, 2 * GROUP, from_next)
    (estimate, sparse, down_sum, right_sum, top_sum, side_sum, down_arg, right_arg, top_arg, side_arg) = outs[:10]
    residuals, new_scalars = outs[10:12]
    members = fit.shape[0]
    shape = (GROUP, cols)
    if first:
        penalty = jnp.ones((1, 1), F32)
        rescale = jnp.ones((1, 1), F32)
    else:
        before, penalty, rescale = new_penalty(scalars, sums)
        old_bound = wide(weight_tv / before, shape)
        old_sparse_bound = wide(weight_sparse / before, shape)
    new_scalars[0:1, :] = wide(penalty, (1, cols))
    new_scalars[1:2, :] = wide(rescale, (1, cols))
    bound = wide(weight_tv / penalty, shape)
    sparse_bound = wide(weight_sparse / penalty, shape)
    scale = wide(rescale, shape)
    has_above, has_below, has_left, has_right = edge_flags()
    lane = lanes_of(shape)
    keep_last = jnp.where(lane == cols - 1, has_right, 1.0)
    is_panel = jnp.where(lane < rows, has_left, 0.0)

    def mixed(a, b):
        return a + scale * b

    def shrunk(value, old, sums_now):
        primal, dual = sums_now
        if first:
            total = value
        else:
            old_total = old
            old_clip = clip(old_total, old_bound)
            total = value + scale * old_clip
        rest = total - clip(total, bound)
        arg = value - rest
        primal = primal + arg * arg
        change = rest if first else rest - (old_total - old_clip)
        dual = dual + change * change
        return total, arg, (primal, dual)

    def step(base, sums_now):
        here = pl.ds(base, GROUP)
        spans = [slice(i * cols, (i + 1) * cols) for i in range(rows)]
        if first:
            now = [fit[here, span] for span in spans]
            near_row = row_halo[here, :]
            near_left, near_right = left_halo[here, :], right_halo[here, :]
        else:
            now = [mixed(fit[here, span], other[here, span]) for span in spans]
            near_row = mixed(row_halo[here, :], row_halo[pl.ds(base + members, GROUP), :])
            near_left = mixed(beside[here, :], roll(beside[here, :], -rows))
            near_right = roll(near_left, -2 * rows)
        column = jnp.zeros(shape, F32)
        for i in range(rows):
            value = now[i]
            estimate[here, spans[i]] = value
            column = jnp.where(lane == i, roll(value, i), column)
            primal, dual = sums_now
            if first:
                total = value
            else:
                old = old_sparse[here, spans[i]]
                total = value + scale * jnp.minimum(old, old_sparse_bound)
            kept = jnp.maximum(total - sparse_bound, 0.0)
            sparse[here, spans[i]] = total
            gap = value - kept
            primal = primal + gap * gap
            change = kept if first else kept - jnp.maximum(old - old_sparse_bound, 0.0)
            dual = dual + change * change
            sums_now = (primal, dual)
            if i < rows - 1:
                diff = now[i + 1] - value
            else:
                diff = (near_row - value) * has_below
            old = None if first else old_down[here, spans[i]]
            total, arg, sums_now = shrunk(diff, old, sums_now)
            down_sum[here, spans[i]] = total
            down_arg[here, spans[i]] = arg
            following = jnp.where(lane == cols - 1, roll(near_right, cols - 1 - i), roll(value, -1))
            diff = (following - value) * keep_last
            old = None if first else old_right[here, spans[i]]
            total, arg, sums_now = shrunk(diff, old, sums_now)
            right_sum[here, spans[i]] = total
            right_arg[here, spans[i]] = arg
        idle = (jnp.zeros(shape, F32),) * 2
        total, arg, _ = shrunk((now[0] - near_row) * has_above, None if first else old_top[here, :], idle)
        top_sum[here, :] = total
        top_arg[here, :] = arg
        panel = jnp.where(lane < rows, column - near_left, 0.0) * is_panel
        total, arg, _ = shrunk(panel, None if first else old_side[here, :], idle)
        side_sum[here, :] = total
        side_arg[here, :] = arg
        return sums_now

    zero = jnp.zeros(shape, F32)
    body, count = groups(members, step)
    primal, dual = lax.fori_loop(0, count, body, (zero, zero), unroll=UNROLL)
    total, cross, weight = quad[0:GROUP, :], quad[GROUP : 2 * GROUP, :], norm[...]
    if not first:
        total = total + scale * (quad[2 * GROUP : 3 * GROUP, :] + scale * quad[4 * GROUP : 5 * GROUP, :])
        cross = cross + scale * quad[3 * GROUP : 4 * GROUP, :]
    square = total + weight
    share = wide(1.0 / (1.0 + penalty), shape)
    part = wide(penalty / (1.0 + penalty), shape)
    if not last:
        outs[12][...] = weight + part * (2.0 * (cross - weight) + part * square)
    residuals[0:GROUP, :] = primal + share * share * square
    residuals[GROUP : 2 * GROUP, :] = dual


def sides_kernel(rows, cols, first, last, *refs):
    (estimate, sparse, down_sum, right_sum, top_sum, side_sum, down_arg, right_arg, top_arg, side_arg) = refs[:10]
    scalars, projected, fit_gram = refs[10:13]
    at = 13
    if not first:
        other_gram, old_multiplier = refs[13:15]
        at = 15
    rhs_high, rhs_low = refs[at : at + 2]
    if not last:
        side, other_side, multiplier = refs[at + 2 :]
    members = estimate.shape[0]
    shape = (GROUP, cols)
    pixels = rows * cols
    penalty, rescale = scalars[0:1, 0:1], scalars[1:2, 0:1]
    bound = wide(weight_tv / penalty, shape)
    sparse_bound = wide(weight_sparse / penalty, shape)
    scale = wide(rescale, shape)
    weight = wide(penalty, shape)
    share = wide(1.0 / (1.0 + penalty), shape)
    lane = lanes_of(shape)

    def step(base, carry):
        here = pl.ds(base, GROUP)
        arg_above, dual_above = top_arg[here, :], clip(top_sum[here, :], bound)
        arg_left, dual_left = side_arg[here, :], clip(side_sum[here, :], bound)
        for i in range(rows):
            span = slice(i * cols, (i + 1) * cols)
            later = slice(pixels + i * cols, pixels + (i + 1) * cols)
            value = estimate[here, span]
            gram = fit_gram[here, span]
            held = gram
            if not first:
                gram = gram + scale * other_gram[here, span]
                held = gram + scale * old_multiplier[here, span]
            data = (projected[here, span] + weight * held) * share
            dual_data = held - data
            down, dual_down = down_arg[here, span], clip(down_sum[here, span], bound)
            right, dual_right = right_arg[here, span], clip(right_sum[here, span], bound)
            beside = jnp.where(lane == 0, roll(arg_left, -i), roll(right, 1))
            dual_beside = jnp.where(lane == 0, roll(dual_left, -i), roll(dual_right, 1))
            total = sparse[here, span]
            rhs = data + jnp.maximum(total - sparse_bound, 0.0) + prox_tau * value - (
                (arg_above - down) + (beside - right)
            )
            rhs_other = -(
                dual_data
                + jnp.minimum(total, sparse_bound)
                + ((dual_above - dual_down) + (dual_beside - dual_right))
            )
            arg_above, dual_above = down, dual_down
            rhs_high[here, span], rhs_low[here, span] = split(rhs)
            rhs_high[here, later], rhs_low[here, later] = split(rhs_other)
            if not last:
                side[here, span] = rhs
                other_side[here, span] = rhs_other
                multiplier[here, span] = dual_data
        return carry

    body, count = groups(members, step)
    lax.fori_loop(0, count, body, 0, unroll=UNROLL)


def solve_kernel(rows, cols, last, *refs):
    inv_high, inv_low, rhs_high, rhs_low = refs[:4]
    if last:
        fit, other = refs[4:]
    else:
        side, other_side, multiplier, projected, scalars = refs[4:9]
        fit, other, fit_gram, other_gram, quad, row_edge, to_pair, to_next, panel = refs[9:]
    members, pixels = fit.shape

    def store(start, size, value):
        if start < pixels:
            fit[:, start : start + size] = value
        else:
            other[:, start - pixels : start - pixels + size] = value

    apply_inverse(inv_high, inv_low, rhs_high, rhs_low, store)
    if last:
        return
    shape = (GROUP, cols)
    weight = wide(scalars[0:1, 0:1], shape)
    below = edge_flags()[1]

    def step(base, sums):
        here = pl.ds(base, GROUP)
        aa, ap, ab, bp, bb = sums
        fits, others = [], []
        for i in range(rows):
            span = slice(i * cols, (i + 1) * cols)
            a, b = fit[here, span], other[here, span]
            ga = side[here, span] - SHIFT * a
            gb = other_side[here, span] - SHIFT * b
            fit_gram[here, span] = ga
            other_gram[here, span] = gb
            target = projected[here, span] + weight * multiplier[here, span]
            aa = aa + a * (ga - 2.0 * target)
            ap = ap + a * target
            ab = ab + b * (2.0 * (ga - target))
            bp = bp + b * target
            bb = bb + b * gb
            fits.append(a)
            others.append(b)
        write_edges(base, members, fits, others, below, row_edge, panel)
        return aa, ap, ab, bp, bb

    zero = jnp.zeros(shape, F32)
    body, count = groups(members, step)
    for index, value in enumerate(lax.fori_loop(0, count, body, (zero,) * 5, unroll=UNROLL)):
        quad[index * GROUP : (index + 1) * GROUP, :] = value
    pack_edges(panel, rows, to_pair, to_next)


def finish_kernel(rows, cols, fit, other, scalars, sums, abundance):
    members = fit.shape[0]
    rescale = new_penalty(scalars, sums)[2]
    scale = wide(rescale, (members, cols))
    for i in range(rows):
        span = slice(i * cols, (i + 1) * cols)
        abundance[pl.ds(i, members, stride=rows), :] = fit[:, span] + scale * other[:, span]


def flat_swap(value, stride, other_row):
    cols = lax.axis_size("col")
    pairs = []
    for row in range(2):
        for col in range(cols):
            target = (1 - row if other_row else row) * cols + (col ^ stride)
            pairs.append((row * cols + col, target))
    return lax.ppermute(value, ("row", "col"), pairs)


def strides():
    cols = lax.axis_size("col")
    return [1 << bit for bit in reversed(range(cols.bit_length() - 1))]


def regular():
    cols = lax.axis_size("col")
    return lax.axis_size("row") == 2 and cols & (cols - 1) == 0


def total_over_mesh(value):
    if not regular():
        return lax.psum(value, ("row", "col"))
    for stride in strides() + [0]:
        value = value + flat_swap(value, stride, True)
    return value


def band_halos(row_edge, columns):
    from_next = next_swap(columns)
    from_pair = pair_swap(columns)
    near_row = flat_swap(row_edge, 0, True)
    return near_row, from_pair, from_next


def pair_swap(value):
    count = lax.axis_size("col")
    return lax.ppermute(value, "col", [(c, c ^ 1) for c in range(count) if c ^ 1 < count])


def next_swap(value):
    count = lax.axis_size("col")
    pairs = []
    for low in range(1, count - 1, 2):
        pairs += [(low, low + 1), (low + 1, low)]
    return lax.ppermute(value, "col", pairs)


def sums_and_halos(value, edges):
    row_edge, to_pair, to_next = edges
    near_row = flat_swap(row_edge, 0, True)
    from_next = next_swap(to_next)
    if not regular():
        from_pair = pair_swap(jnp.concatenate([value, to_pair], axis=0))
        return lax.psum(value, ("row", "col")), near_row, from_pair, from_next
    stages = strides()
    for stride in stages[:-1]:
        value = value + flat_swap(value, stride, True)
    from_pair = flat_swap(jnp.concatenate([value, to_pair], axis=0), stages[-1], False)
    value = value + from_pair[: value.shape[0], :]
    value = value + flat_swap(value, 0, True)
    return value, near_row, from_pair, from_next


def gathered(library):
    half_rows = library.shape[0] // 2
    if not regular() or half_rows % 16 or lax.axis_size("col") < 2:
        return [lax.all_gather(library, "col", axis=0, tiled=True)], True
    parity = lax.axis_index("row")
    bits = lax.axis_index("col")
    for _ in strides():
        parity = parity ^ (bits & 1)
        bits = bits >> 1
    mine = lax.dynamic_slice_in_dim(library, parity * half_rows, half_rows, 0)
    tag = mine
    order = strides()
    reach = [0]
    for stride in order[:-1]:
        got = flat_swap(mine, stride, True)
        mine = jnp.concatenate([mine, got], axis=0)
        reach = reach + [r ^ stride for r in reach]
    rest = flat_swap(mine, order[-1], True)
    reach = reach + [r ^ order[-1] for r in reach]
    other = flat_swap(mine, 0, True)
    other_rest = flat_swap(rest, 0, True)
    return [mine, rest, other, other_rest, tag], reach


def iterate(observed, library):
    channels, rows, cols = observed.shape
    members = library.shape[1]
    pixels = rows * cols
    field = ((members, pixels), F32)
    strip = ((members, cols), F32)
    scalar = ((GROUP, cols), F32)
    pieces, order = gathered(library)
    flat, columns, row_edge, norm = call(
        functools.partial(survey_kernel, rows, cols),
        [((channels, pixels), BF16), ((2 * rows, channels), BF16), ((channels, cols), BF16), scalar],
        [observed.reshape(channels * rows, cols)],
        [
            pltpu.VMEM((channels * rows, cols), BF16),
            pltpu.VMEM((channels * rows, cols), F32),
            pltpu.SemaphoreType.DMA((4,)),
        ],
        space=pltpu.HBM,
        limit=50,
        flops=2 * rows * channels * pixels,
    )
    near = band_halos(row_edge, columns)
    half = ((members, members), BF16)
    extended = pltpu.VMEM((members, pixels + 2 * cols), BF16)
    scratch = [
        pltpu.VMEM((members, members), F32),
        pltpu.VMEM((members, members), F32),
        extended,
        extended,
        pltpu.SMEM((2,), F32),
        pltpu.VMEM((cols, channels), BF16),
    ]
    work = 2 * members * members * pixels
    if order is not True:
        parts = [pltpu.VMEM((channels // 2, members), BF16), pltpu.VMEM((channels // 2, pixels), BF16)]
        scratch += [pltpu.VMEM((channels, members), BF16), *parts]
        pieces += call(
            functools.partial(early_kernel, order[: len(order) // 2]),
            [field, ((members, members), F32)],
            [flat, pieces[0], pieces[2]],
            parts,
            flops=4 * work,
        )
    projected, inv_high, inv_low, fit, fit_gram, quad, *near = call(
        functools.partial(start_kernel, rows, cols, order),
        [field, half, half, field, field, ((2 * GROUP, cols), F32), strip, strip, strip],
        [flat, *near, *pieces],
        scratch,
        flops=8 * work,
    )
    state = None
    other = other_gram = multiplier = scalars = sums = None
    for iteration in range(ITERS):
        first = iteration == 0
        last = iteration == ITERS - 1
        if first:
            args = [fit, quad, norm, *near]
        else:
            args = [fit, other, quad, norm, *near, scalars, sums, *state[1:6]]
        results = call(
            functools.partial(shrink_kernel, rows, cols, first, last),
            [field] * 4 + [strip] * 2 + [field] * 2 + [strip] * 2
            + [((2 * GROUP, cols), F32), scalar] + ([] if last else [scalar]),
            args,
            [] if first else [pltpu.VMEM(*strip)],
            flops=work,
        )
        state, residuals, scalars = results[:10], results[10], results[11]
        if last:
            sums = total_over_mesh(residuals)
        args = [*state, scalars, projected, fit_gram]
        if not first:
            args += [other_gram, multiplier]
        wide_half = ((members, 2 * pixels), BF16)
        rhs_high, rhs_low, *sides = call(
            functools.partial(sides_kernel, rows, cols, first, last),
            [wide_half] * 2 + ([] if last else [field] * 3),
            args,
            flops=2 * work,
        )
        packed = ((2 * rows * members // cols, cols), F32)
        if last:
            outs, more = [], []
        else:
            multiplier = sides[2]
            outs = [field] * 2 + [((5 * GROUP, cols), F32), ((2 * members, cols), F32), packed, packed]
            more = [*sides, projected, scalars]
        results_of = call(
            functools.partial(solve_kernel, rows, cols, last),
            [field] * 2 + outs,
            [inv_high, inv_low, rhs_high, rhs_low, *more],
            [] if last else [pltpu.VMEM(*strip)],
            flops=2 * work,
        )
        fit, other = results_of[:2]
        if last:
            break
        fit_gram, other_gram, quad, *edge = results_of[2:]
        sums, *near = sums_and_halos(residuals, edge)
        norm = results[12]
    (abundance,) = call(
        functools.partial(finish_kernel, rows, cols),
        [((members * rows, cols), F32)],
        [fit, other, scalars, sums],
        flops=work // 8,
    )
    return abundance.reshape(members, rows, cols)


def solution(mesh):
    return jax.shard_map(
        iterate,
        mesh=mesh,
        in_specs=(P(None, "row", "col"), P("col", None)),
        out_specs=P(None, "row", "col"),
        check_vma=False,
    )
```

```python
import functools

import jax
import jax.numpy as jnp
from jax import lax
from jax.experimental import pallas as pl
from jax.experimental.pallas import tpu as pltpu
from jax.sharding import PartitionSpec as P


ITERS = 3

prox_tau = 8.0
weight_sparse = 0.3
weight_tv = 1.0

F32 = jnp.float32
BF16 = jnp.bfloat16
SHIFT = 1.0 + prox_tau
GROUP = 8
UNROLL = 16


def split(value):
    high = value.astype(BF16)
    return high, (value - high.astype(F32)).astype(BF16)


def dot(left, right):
    return jnp.dot(left, right, preferred_element_type=F32)


def dot_full(left, right):
    return jnp.dot(left, right, precision=lax.Precision.HIGHEST, preferred_element_type=F32)


def dot_columns(left, right):
    return lax.dot_general(left, right, (((0,), (0,)), ((), ())), preferred_element_type=F32)


def clip(value, bound):
    return jnp.minimum(jnp.maximum(value, -bound), bound)


def call(body, outs, args, scratch=(), flops=0, limit=24, space=pltpu.VMEM):
    return pl.pallas_call(
        body,
        out_shape=[jax.ShapeDtypeStruct(*out) for out in outs],
        in_specs=[pl.BlockSpec(memory_space=space)] * len(args),
        out_specs=[pl.BlockSpec(memory_space=pltpu.VMEM)] * len(outs),
        scratch_shapes=list(scratch),
        cost_estimate=pl.CostEstimate(flops=flops, bytes_accessed=0, transcendentals=0),
        compiler_params=pltpu.CompilerParams(vmem_limit_bytes=limit << 20),
    )(*args)


def groups(members, step):
    def body(index, carry):
        return step(pl.multiple_of(index * GROUP, GROUP), carry)

    return body, members // GROUP


def roll(value, shift):
    return pltpu.roll(value, shift % value.shape[1], 1)


def lanes_of(shape):
    return lax.broadcasted_iota(jnp.int32, shape, 1)


def flag(condition):
    return jnp.where(condition, 1.0, 0.0).astype(F32)


def edge_flags():
    row, col = lax.axis_index("row"), lax.axis_index("col")
    return (
        flag(row > 0),
        flag(row < lax.axis_size("row") - 1),
        flag(col > 0),
        flag(col < lax.axis_size("col") - 1),
    )


def invert(gram, inverse, power, left):
    eye = flag(
        lax.broadcasted_iota(jnp.int32, gram.shape, 0) == lax.broadcasted_iota(jnp.int32, gram.shape, 1)
    )
    system = gram + SHIFT * eye
    bound = jnp.max(jnp.sum(jnp.abs(gram), axis=1, keepdims=True)) + SHIFT
    nearest = jnp.sum(system * eye) / jnp.sum(system * system)
    scale = jnp.where(nearest * bound < 1.9, nearest, 2.0 / (bound + SHIFT))
    first = eye - scale * system
    squared = dot_full(first, first)
    inverse[...] = scale * (eye + first)
    power[...] = squared
    left[0] = jnp.sum(squared * squared)

    def step(index, carry):
        @pl.when(left[0] > 0.0)
        def _():
            current = power[...]
            inverse[...] = inverse[...] + dot_full(inverse[...], current)

        @pl.when(left[0] > 1e-6)
        def _():
            current = power[...]
            squared = dot_full(current, current)
            power[...] = squared
            left[1] = jnp.sum(squared * squared)

        left[0] = jnp.where(left[0] > 1e-6, left[1], 0.0)
        return carry

    lax.fori_loop(0, 20, step, 0)


def apply_inverse(inv_high, inv_low, rhs_high, rhs_low, store):
    width = rhs_high.shape[1]
    for start in range(0, width, 512):
        block = min(512, width - start)
        high, low = rhs_high[:, start : start + block], rhs_low[:, start : start + block]
        store(start, block, dot(inv_high[...], high) + (dot(inv_high[...], low) + dot(inv_low[...], high)))


def survey_kernel(rows, cols, observed, flat, columns, row_edge, norm, band, wide_band, arrived):
    channels, pixels = flat.shape
    tall = 2 * GROUP
    zero = jnp.zeros((tall, cols), F32)
    parts = arrived.shape[0]
    size = channels * rows // parts
    copies = []
    for part in range(parts):
        here = pl.ds(part * size, size)
        copies.append(pltpu.make_async_copy(observed.at[here, :], band.at[here, :], arrived.at[part]))
        copies[-1].start()

    def widen(index, total):
        total = list(total)
        for part in range(rows):
            here = pl.ds(pl.multiple_of((index * rows + part) * tall, tall), tall)
            value = band[here, :].astype(F32)
            wide_band[here, :] = value
            total[part % 2] = total[part % 2] + value * value
        return tuple(total)

    total = (zero, zero)
    steps = channels // tall // parts
    for part in range(parts):
        copies[part].wait()
        total = lax.fori_loop(part * steps, (part + 1) * steps, widen, total, unroll=4)
    total = total[0] + total[1]
    norm[...] = total[:GROUP, :] + total[GROUP:, :]

    def place(index, carry):
        start = pl.multiple_of(index * tall, tall)
        for i in range(rows):
            value = wide_band[pl.ds(start * rows + i, tall, stride=rows), :]
            flat[pl.ds(start, tall), i * cols : (i + 1) * cols] = value.astype(BF16)
        return carry

    lax.fori_loop(0, channels // tall, place, 0, unroll=4)
    spot = lax.broadcasted_iota(jnp.int32, (2 * rows, pixels), 0)
    pixel = lax.broadcasted_iota(jnp.int32, (2 * rows, pixels), 1)
    wanted = jnp.where(spot < rows, spot * cols, (spot - rows) * cols + cols - 1)
    chosen = flag(pixel == wanted).astype(BF16)
    columns[...] = lax.dot_general(
        chosen, flat[...], (((1,), (1,)), ((), ())), preferred_element_type=F32
    ).astype(BF16)
    is_upper = edge_flags()[1] > 0.0

    @pl.when(is_upper)
    def _():
        row_edge[...] = flat[:, pixels - cols :]

    @pl.when(jnp.logical_not(is_upper))
    def _():
        row_edge[...] = flat[:, :cols]


def gather_half(observed, first_half, second_half, order, half, library_part, band_part):
    blocks = len(order)
    rows = first_half.shape[0] // blocks
    own = lax.axis_index("col")
    for block in range(blocks):
        at = block * 2 * rows
        source = slice(block * rows, (block + 1) * rows)
        library_part[pl.ds(pl.multiple_of(at + half * rows, rows), rows), :] = first_half[source, :]
        library_part[pl.ds(pl.multiple_of(at + (1 - half) * rows, rows), rows), :] = second_half[source, :]
        base = pl.multiple_of((own ^ order[block]) * (2 * rows), 2 * rows)
        band_part[at : at + 2 * rows, :] = observed[pl.ds(base, 2 * rows), :]


def own_half():
    parity = lax.axis_index("row")
    bits = lax.axis_index("col")
    for _ in range(max(1, (lax.axis_size("col") - 1).bit_length())):
        parity = parity ^ (bits & 1)
        bits = bits >> 1
    return parity


def early_kernel(order, observed, mine, other, projected, gram, library_part, band_part):
    gather_half(observed, mine, other, order, own_half(), library_part, band_part)
    pixels = band_part.shape[1]
    for start in range(0, pixels, 512):
        span = slice(start, min(start + 512, pixels))
        projected[:, span] = dot_columns(library_part[...], band_part[:, span])
    gram[...] = dot_columns(library_part[...], library_part[...])


def start_kernel(rows, cols, order, *refs):
    ordered = order is True
    observed, row_halo, from_pair, from_next = refs[:4]
    inputs = 5 if ordered else 11
    pieces = refs[4:inputs]
    projected, inv_high, inv_low, fit, fit_gram, quad, near_row, near_left, near_right = refs[inputs : inputs + 9]
    inverse, power, rhs_high, rhs_low, left, panel = refs[inputs + 9 : inputs + 15]
    if ordered:
        full = pieces[0]
    else:
        full, library_part, band_part = refs[inputs + 15 :]
        place_library(pieces[:5], full, order)
        early, early_gram = pieces[5:]
        late = order[len(order) // 2 :]
        gather_half(observed, pieces[1], pieces[3], late, own_half(), library_part, band_part)
    members = full.shape[1]
    pixels = rows * cols
    panel[...] = jnp.zeros(panel.shape, BF16)
    is_odd = (lax.axis_index("col") & 1) > 0
    for low, odd_one, even_one in ((0, from_next, from_pair), (2 * rows, from_pair, from_next)):

        @pl.when(is_odd)
        def _():
            panel[low : low + 2 * rows, :] = odd_one[...]

        @pl.when(jnp.logical_not(is_odd))
        def _():
            panel[low : low + 2 * rows, :] = even_one[...]

    block = min(512, pixels)
    for start in range(0, pixels, block):
        span = slice(start, start + block)
        if ordered:
            result = dot_columns(full[...], observed[:, span])
        else:
            result = early[:, span] + dot_columns(library_part[...], band_part[:, span])
        projected[:, span] = result
        rhs_high[:, span], rhs_low[:, span] = split(result)
    span = slice(pixels, pixels + cols)
    rhs_high[:, span], rhs_low[:, span] = split(dot_columns(full[...], row_halo[...]))
    span = slice(pixels + cols, pixels + cols + panel.shape[0])
    beside = lax.dot_general(full[...], panel[...], (((0,), (1,)), ((), ())), preferred_element_type=F32)
    rhs_high[:, span], rhs_low[:, span] = split(beside)
    if ordered:
        gram = dot_columns(full[...], full[...])
    else:
        gram = early_gram[...] + dot_columns(library_part[...], library_part[...])
    invert(gram, inverse, power, left)
    inv_high[...], inv_low[...] = split(inverse[...])

    def store(start, size, value):
        if start < pixels:
            fit[:, start : start + size] = value
        else:
            near_row[...] = value[:, :cols]
            near_right[...] = value[:, cols:]
            near_left[...] = roll(value[:, cols:], -3 * rows)

    apply_inverse(inv_high, inv_low, rhs_high, rhs_low, store)

    def step(base, sums):
        here = pl.ds(base, GROUP)
        total, cross = sums
        for i in range(rows):
            span = slice(i * cols, (i + 1) * cols)
            a, p = fit[here, span], projected[here, span]
            ga = p - SHIFT * a
            fit_gram[here, span] = ga
            total = total + a * (ga - 2.0 * p)
            cross = cross + a * p
        return total, cross

    zero = jnp.zeros((GROUP, cols), F32)
    body, count = groups(members, step)
    total, cross = lax.fori_loop(0, count, body, (zero, zero), unroll=UNROLL)
    quad[0:GROUP, :] = total
    quad[GROUP : 2 * GROUP, :] = cross


def write_edges(base, members, a, b, below, row_edge, panel):
    here = pl.ds(base, GROUP)
    is_upper = below > 0.0
    row_edge[here, :] = jnp.where(is_upper, a[-1], a[0])
    row_edge[pl.ds(base + members, GROUP), :] = jnp.where(is_upper, b[-1], b[0])
    lane = lanes_of(a[0].shape)
    cols = a[0].shape[1]
    count = len(a) + len(b)
    shown = jnp.zeros_like(a[0])
    for i, value in enumerate(a + b):
        shown = jnp.where(lane == i, roll(value, i), shown)
        shown = jnp.where(lane == count + i, roll(value, count + i + 1 - cols), shown)
    panel[here, :] = shown


def pack_edges(panel, rows, to_pair, to_next):
    members, cols = panel.shape
    count = 2 * rows
    is_odd = (lax.axis_index("col") & 1) > 0
    for part in range(members // cols):
        turned = jnp.transpose(panel[part * cols : (part + 1) * cols, :])
        first, final = turned[:count, :], turned[count : 2 * count, :]
        here = slice(part * count, (part + 1) * count)
        to_pair[here, :] = jnp.where(is_odd, first, final)
        to_next[here, :] = jnp.where(is_odd, final, first)


def unpack_edges(panel, rows, from_pair, skip, from_next):
    members, cols = panel.shape
    count = 2 * rows
    is_odd = (lax.axis_index("col") & 1) > 0
    rest = jnp.zeros((cols - 2 * count, cols), F32)
    for part in range(members // cols):
        pair = from_pair[skip + part * count : skip + (part + 1) * count, :]
        other = from_next[part * count : (part + 1) * count, :]
        on_left, on_right = jnp.where(is_odd, pair, other), jnp.where(is_odd, other, pair)
        panel[part * cols : (part + 1) * cols, :] = jnp.transpose(
            jnp.concatenate([on_left, on_right, rest], axis=0)
        )


def place_library(pieces, full, order):
    mine, mine_rest, other, other_rest, rows_of = pieces
    rows = rows_of.shape[0]
    own = lax.axis_index("col")
    parity = lax.axis_index("row")
    bits = own
    for _ in range(max(1, (lax.axis_size("col") - 1).bit_length())):
        parity = parity ^ (bits & 1)
        bits = bits >> 1
    half = parity
    blocks = mine.shape[0] // rows
    for offset, first, second in ((0, mine, other), (blocks, mine_rest, other_rest)):
        for block in range(blocks):
            base = (own ^ order[block + offset]) * (2 * rows)
            source = slice(block * rows, (block + 1) * rows)
            full[pl.ds(pl.multiple_of(base + half * rows, rows), rows), :] = first[source, :]
            full[pl.ds(pl.multiple_of(base + (1 - half) * rows, rows), rows), :] = second[source, :]


def new_penalty(scalars, sums):
    penalty = scalars[0:1, 0:1]
    primal = jnp.sum(jnp.sum(sums[0:GROUP, :], axis=0, keepdims=True), axis=1, keepdims=True)
    dual = jnp.sum(jnp.sum(sums[GROUP : 2 * GROUP, :], axis=0, keepdims=True), axis=1, keepdims=True)
    following = penalty * jnp.sqrt(jnp.sqrt((primal + 1.0) / (penalty * penalty * dual + 1.0)))
    return penalty, following, penalty / following


def wide(value, shape):
    return jnp.broadcast_to(value, shape)


def shrink_kernel(rows, cols, first, last, *refs):
    if first:
        fit, quad, norm, row_halo, left_halo, right_halo = refs[:6]
        outs = refs[6:]
    else:
        (fit, other, quad, norm, row_halo, from_pair, from_next, scalars, sums) = refs[:9]
        (old_sparse, old_down, old_right, old_top, old_side) = refs[9:14]
        outs = refs[14:]
        beside = outs[-1]
        unpack_edges(beside, rows, from_pair, 2 * GROUP, from_next)
    (estimate, sparse, down_sum, right_sum, top_sum, side_sum, down_arg, right_arg, top_arg, side_arg) = outs[:10]
    residuals, new_scalars = outs[10:12]
    members = fit.shape[0]
    shape = (GROUP, cols)
    if first:
        penalty = jnp.ones((1, 1), F32)
        rescale = jnp.ones((1, 1), F32)
    else:
        before, penalty, rescale = new_penalty(scalars, sums)
        old_bound = wide(weight_tv / before, shape)
        old_sparse_bound = wide(weight_sparse / before, shape)
    new_scalars[0:1, :] = wide(penalty, (1, cols))
    new_scalars[1:2, :] = wide(rescale, (1, cols))
    bound = wide(weight_tv / penalty, shape)
    sparse_bound = wide(weight_sparse / penalty, shape)
    scale = wide(rescale, shape)
    has_above, has_below, has_left, has_right = edge_flags()
    lane = lanes_of(shape)
    keep_last = jnp.where(lane == cols - 1, has_right, 1.0)
    is_panel = jnp.where(lane < rows, has_left, 0.0)

    def mixed(a, b):
        return a + scale * b

    def shrunk(value, old, sums_now):
        primal, dual = sums_now
        if first:
            total = value
        else:
            old_total = old
            old_clip = clip(old_total, old_bound)
            total = value + scale * old_clip
        rest = total - clip(total, bound)
        arg = value - rest
        primal = primal + arg * arg
        change = rest if first else rest - (old_total - old_clip)
        dual = dual + change * change
        return total, arg, (primal, dual)

    def step(base, sums_now):
        here = pl.ds(base, GROUP)
        spans = [slice(i * cols, (i + 1) * cols) for i in range(rows)]
        if first:
            now = [fit[here, span] for span in spans]
            near_row = row_halo[here, :]
            near_left, near_right = left_halo[here, :], right_halo[here, :]
        else:
            now = [mixed(fit[here, span], other[here, span]) for span in spans]
            near_row = mixed(row_halo[here, :], row_halo[pl.ds(base + members, GROUP), :])
            near_left = mixed(beside[here, :], roll(beside[here, :], -rows))
            near_right = roll(near_left, -2 * rows)
        column = jnp.zeros(shape, F32)
        for i in range(rows):
            value = now[i]
            estimate[here, spans[i]] = value
            column = jnp.where(lane == i, roll(value, i), column)
            primal, dual = sums_now
            if first:
                total = value
            else:
                old = old_sparse[here, spans[i]]
                total = value + scale * jnp.minimum(old, old_sparse_bound)
            kept = jnp.maximum(total - sparse_bound, 0.0)
            sparse[here, spans[i]] = total
            gap = value - kept
            primal = primal + gap * gap
            change = kept if first else kept - jnp.maximum(old - old_sparse_bound, 0.0)
            dual = dual + change * change
            sums_now = (primal, dual)
            if i < rows - 1:
                diff = now[i + 1] - value
            else:
                diff = (near_row - value) * has_below
            old = None if first else old_down[here, spans[i]]
            total, arg, sums_now = shrunk(diff, old, sums_now)
            down_sum[here, spans[i]] = total
            down_arg[here, spans[i]] = arg
            following = jnp.where(lane == cols - 1, roll(near_right, cols - 1 - i), roll(value, -1))
            diff = (following - value) * keep_last
            old = None if first else old_right[here, spans[i]]
            total, arg, sums_now = shrunk(diff, old, sums_now)
            right_sum[here, spans[i]] = total
            right_arg[here, spans[i]] = arg
        idle = (jnp.zeros(shape, F32),) * 2
        total, arg, _ = shrunk((now[0] - near_row) * has_above, None if first else old_top[here, :], idle)
        top_sum[here, :] = total
        top_arg[here, :] = arg
        panel = jnp.where(lane < rows, column - near_left, 0.0) * is_panel
        total, arg, _ = shrunk(panel, None if first else old_side[here, :], idle)
        side_sum[here, :] = total
        side_arg[here, :] = arg
        return sums_now

    zero = jnp.zeros(shape, F32)
    body, count = groups(members, step)
    primal, dual = lax.fori_loop(0, count, body, (zero, zero), unroll=UNROLL)
    total, cross, weight = quad[0:GROUP, :], quad[GROUP : 2 * GROUP, :], norm[...]
    if not first:
        total = total + scale * (quad[2 * GROUP : 3 * GROUP, :] + scale * quad[4 * GROUP : 5 * GROUP, :])
        cross = cross + scale * quad[3 * GROUP : 4 * GROUP, :]
    square = total + weight
    share = wide(1.0 / (1.0 + penalty), shape)
    part = wide(penalty / (1.0 + penalty), shape)
    if not last:
        outs[12][...] = weight + part * (2.0 * (cross - weight) + part * square)
    residuals[0:GROUP, :] = primal + share * share * square
    residuals[GROUP : 2 * GROUP, :] = dual


def sides_kernel(rows, cols, first, last, *refs):
    (estimate, sparse, down_sum, right_sum, top_sum, side_sum, down_arg, right_arg, top_arg, side_arg) = refs[:10]
    scalars, projected, fit_gram = refs[10:13]
    at = 13
    if not first:
        other_gram, old_multiplier = refs[13:15]
        at = 15
    rhs_high, rhs_low = refs[at : at + 2]
    if not last:
        side, other_side, multiplier = refs[at + 2 :]
    members = estimate.shape[0]
    shape = (GROUP, cols)
    pixels = rows * cols
    penalty, rescale = scalars[0:1, 0:1], scalars[1:2, 0:1]
    bound = wide(weight_tv / penalty, shape)
    sparse_bound = wide(weight_sparse / penalty, shape)
    scale = wide(rescale, shape)
    weight = wide(penalty, shape)
    share = wide(1.0 / (1.0 + penalty), shape)
    lane = lanes_of(shape)

    def step(base, carry):
        here = pl.ds(base, GROUP)
        arg_above, dual_above = top_arg[here, :], clip(top_sum[here, :], bound)
        arg_left, dual_left = side_arg[here, :], clip(side_sum[here, :], bound)
        for i in range(rows):
            span = slice(i * cols, (i + 1) * cols)
            later = slice(pixels + i * cols, pixels + (i + 1) * cols)
            value = estimate[here, span]
            gram = fit_gram[here, span]
            held = gram
            if not first:
                gram = gram + scale * other_gram[here, span]
                held = gram + scale * old_multiplier[here, span]
            data = (projected[here, span] + weight * held) * share
            dual_data = held - data
            down, dual_down = down_arg[here, span], clip(down_sum[here, span], bound)
            right, dual_right = right_arg[here, span], clip(right_sum[here, span], bound)
            beside = jnp.where(lane == 0, roll(arg_left, -i), roll(right, 1))
            dual_beside = jnp.where(lane == 0, roll(dual_left, -i), roll(dual_right, 1))
            total = sparse[here, span]
            rhs = data + jnp.maximum(total - sparse_bound, 0.0) + prox_tau * value - (
                (arg_above - down) + (beside - right)
            )
            rhs_other = -(
                dual_data
                + jnp.minimum(total, sparse_bound)
                + ((dual_above - dual_down) + (dual_beside - dual_right))
            )
            arg_above, dual_above = down, dual_down
            rhs_high[here, span], rhs_low[here, span] = split(rhs)
            rhs_high[here, later], rhs_low[here, later] = split(rhs_other)
            if not last:
                side[here, span] = rhs
                other_side[here, span] = rhs_other
                multiplier[here, span] = dual_data
        return carry

    body, count = groups(members, step)
    lax.fori_loop(0, count, body, 0, unroll=UNROLL)


def solve_kernel(inv_high, inv_low, rhs_high, rhs_low, fit, other):
    pixels = fit.shape[1]

    def store(start, size, value):
        if start < pixels:
            fit[:, start : start + size] = value
        else:
            other[:, start - pixels : start - pixels + size] = value

    apply_inverse(inv_high, inv_low, rhs_high, rhs_low, store)


def products_kernel(rows, cols, *refs):
    fit, other, side, other_side, multiplier, projected, scalars = refs[:7]
    fit_gram, other_gram, quad, row_edge, to_pair, to_next, panel = refs[7:]
    members = fit.shape[0]
    shape = (GROUP, cols)
    weight = wide(scalars[0:1, 0:1], shape)
    below = edge_flags()[1]

    def step(base, sums):
        here = pl.ds(base, GROUP)
        aa, ap, ab, bp, bb = sums
        fits, others = [], []
        for i in range(rows):
            span = slice(i * cols, (i + 1) * cols)
            a, b = fit[here, span], other[here, span]
            ga = side[here, span] - SHIFT * a
            gb = other_side[here, span] - SHIFT * b
            fit_gram[here, span] = ga
            other_gram[here, span] = gb
            target = projected[here, span] + weight * multiplier[here, span]
            aa = aa + a * (ga - 2.0 * target)
            ap = ap + a * target
            ab = ab + b * (2.0 * (ga - target))
            bp = bp + b * target
            bb = bb + b * gb
            fits.append(a)
            others.append(b)
        write_edges(base, members, fits, others, below, row_edge, panel)
        return aa, ap, ab, bp, bb

    zero = jnp.zeros(shape, F32)
    body, count = groups(members, step)
    for index, value in enumerate(lax.fori_loop(0, count, body, (zero,) * 5, unroll=UNROLL)):
        quad[index * GROUP : (index + 1) * GROUP, :] = value
    pack_edges(panel, rows, to_pair, to_next)


def finish_kernel(rows, cols, fit, other, scalars, sums, abundance):
    members = fit.shape[0]
    rescale = new_penalty(scalars, sums)[2]
    scale = wide(rescale, (members, cols))
    for i in range(rows):
        span = slice(i * cols, (i + 1) * cols)
        abundance[pl.ds(i, members, stride=rows), :] = fit[:, span] + scale * other[:, span]


def flat_swap(value, stride, other_row):
    cols = lax.axis_size("col")
    pairs = []
    for row in range(2):
        for col in range(cols):
            target = (1 - row if other_row else row) * cols + (col ^ stride)
            pairs.append((row * cols + col, target))
    return lax.ppermute(value, ("row", "col"), pairs)


def strides():
    cols = lax.axis_size("col")
    return [1 << bit for bit in reversed(range(cols.bit_length() - 1))]


def regular():
    cols = lax.axis_size("col")
    return lax.axis_size("row") == 2 and cols & (cols - 1) == 0


def total_over_mesh(value):
    if not regular():
        return lax.psum(value, ("row", "col"))
    for stride in strides() + [0]:
        value = value + flat_swap(value, stride, True)
    return value


def band_halos(row_edge, columns):
    from_next = next_swap(columns)
    from_pair = pair_swap(columns)
    near_row = flat_swap(row_edge, 0, True)
    return near_row, from_pair, from_next


def pair_swap(value):
    count = lax.axis_size("col")
    return lax.ppermute(value, "col", [(c, c ^ 1) for c in range(count) if c ^ 1 < count])


def next_swap(value):
    count = lax.axis_size("col")
    pairs = []
    for low in range(1, count - 1, 2):
        pairs += [(low, low + 1), (low + 1, low)]
    return lax.ppermute(value, "col", pairs)


def sums_and_halos(value, edges):
    row_edge, to_pair, to_next = edges
    near_row = flat_swap(row_edge, 0, True)
    from_next = next_swap(to_next)
    if not regular():
        from_pair = pair_swap(jnp.concatenate([value, to_pair], axis=0))
        return lax.psum(value, ("row", "col")), near_row, from_pair, from_next
    stages = strides()
    for stride in stages[:-1]:
        value = value + flat_swap(value, stride, True)
    from_pair = flat_swap(jnp.concatenate([value, to_pair], axis=0), stages[-1], False)
    value = value + from_pair[: value.shape[0], :]
    value = value + flat_swap(value, 0, True)
    return value, near_row, from_pair, from_next


def gathered(library):
    half_rows = library.shape[0] // 2
    if not regular() or half_rows % 16 or lax.axis_size("col") < 2:
        return [lax.all_gather(library, "col", axis=0, tiled=True)], True
    parity = lax.axis_index("row")
    bits = lax.axis_index("col")
    for _ in strides():
        parity = parity ^ (bits & 1)
        bits = bits >> 1
    mine = lax.dynamic_slice_in_dim(library, parity * half_rows, half_rows, 0)
    tag = mine
    order = strides()
    reach = [0]
    for stride in order[:-1]:
        got = flat_swap(mine, stride, True)
        mine = jnp.concatenate([mine, got], axis=0)
        reach = reach + [r ^ stride for r in reach]
    rest = flat_swap(mine, order[-1], True)
    reach = reach + [r ^ order[-1] for r in reach]
    other = flat_swap(mine, 0, True)
    other_rest = flat_swap(rest, 0, True)
    return [mine, rest, other, other_rest, tag], reach


def iterate(observed, library):
    channels, rows, cols = observed.shape
    members = library.shape[1]
    pixels = rows * cols
    field = ((members, pixels), F32)
    strip = ((members, cols), F32)
    scalar = ((GROUP, cols), F32)
    pieces, order = gathered(library)
    flat, columns, row_edge, norm = call(
        functools.partial(survey_kernel, rows, cols),
        [((channels, pixels), BF16), ((2 * rows, channels), BF16), ((channels, cols), BF16), scalar],
        [observed.reshape(channels * rows, cols)],
        [
            pltpu.VMEM((channels * rows, cols), BF16),
            pltpu.VMEM((channels * rows, cols), F32),
            pltpu.SemaphoreType.DMA((4,)),
        ],
        space=pltpu.HBM,
        limit=50,
        flops=2 * rows * channels * pixels,
    )
    near = band_halos(row_edge, columns)
    half = ((members, members), BF16)
    extended = pltpu.VMEM((members, pixels + 2 * cols), BF16)
    scratch = [
        pltpu.VMEM((members, members), F32),
        pltpu.VMEM((members, members), F32),
        extended,
        extended,
        pltpu.SMEM((2,), F32),
        pltpu.VMEM((cols, channels), BF16),
    ]
    work = 2 * members * members * pixels
    if order is not True:
        parts = [pltpu.VMEM((channels // 2, members), BF16), pltpu.VMEM((channels // 2, pixels), BF16)]
        scratch += [pltpu.VMEM((channels, members), BF16), *parts]
        pieces += call(
            functools.partial(early_kernel, order[: len(order) // 2]),
            [field, ((members, members), F32)],
            [flat, pieces[0], pieces[2]],
            parts,
            flops=4 * work,
        )
    projected, inv_high, inv_low, fit, fit_gram, quad, *near = call(
        functools.partial(start_kernel, rows, cols, order),
        [field, half, half, field, field, ((2 * GROUP, cols), F32), strip, strip, strip],
        [flat, *near, *pieces],
        scratch,
        flops=8 * work,
    )
    state = None
    other = other_gram = multiplier = scalars = sums = None
    for iteration in range(ITERS):
        first = iteration == 0
        last = iteration == ITERS - 1
        if first:
            args = [fit, quad, norm, *near]
        else:
            args = [fit, other, quad, norm, *near, scalars, sums, *state[1:6]]
        results = call(
            functools.partial(shrink_kernel, rows, cols, first, last),
            [field] * 4 + [strip] * 2 + [field] * 2 + [strip] * 2
            + [((2 * GROUP, cols), F32), scalar] + ([] if last else [scalar]),
            args,
            [] if first else [pltpu.VMEM(*strip)],
            flops=work,
        )
        state, residuals, scalars = results[:10], results[10], results[11]
        if last:
            sums = total_over_mesh(residuals)
        args = [*state, scalars, projected, fit_gram]
        if not first:
            args += [other_gram, multiplier]
        wide_half = ((members, 2 * pixels), BF16)
        rhs_high, rhs_low, *sides = call(
            functools.partial(sides_kernel, rows, cols, first, last),
            [wide_half] * 2 + ([] if last else [field] * 3),
            args,
            flops=2 * work,
        )
        packed = ((2 * rows * members // cols, cols), F32)
        fit, other = call(solve_kernel, [field] * 2, [inv_high, inv_low, rhs_high, rhs_low], flops=2 * work)
        if last:
            break
        multiplier = sides[2]
        fit_gram, other_gram, quad, *edge = call(
            functools.partial(products_kernel, rows, cols),
            [field] * 2 + [((5 * GROUP, cols), F32), ((2 * members, cols), F32), packed, packed],
            [fit, other, *sides, projected, scalars],
            [pltpu.VMEM(*strip)],
            flops=2 * work,
        )
        sums, *near = sums_and_halos(residuals, edge)
        norm = results[12]
    (abundance,) = call(
        functools.partial(finish_kernel, rows, cols),
        [((members * rows, cols), F32)],
        [fit, other, scalars, sums],
        flops=work // 8,
    )
    return abundance.reshape(members, rows, cols)


def solution(mesh):
    return jax.shard_map(
        iterate,
        mesh=mesh,
        in_specs=(P(None, "row", "col"), P("col", None)),
        out_specs=P(None, "row", "col"),
        check_vma=False,
    )
```
